8 devices in a mesh: rep: 1 (over z), dp: 2 (over y), sp: 4 (over x, core).
Axes of the slice: x: 2, y: 2, z: 1, core: 2. Of those that a mesh axis runs over, the one named last changes fastest.
Arguments:
- hidden: bfloat16 [128, 4096], P(('rep', 'dp'))
- w_query: bfloat16 [4096, 4096], replicated
- w_key: bfloat16 [4096, 256], replicated
- w_value: bfloat16 [4096, 256], replicated
- w_out: bfloat16 [4096, 4096], P('sp')
- k_cache: bfloat16 [128, 1024, 1, 256], P(('rep', 'dp'), 'sp')
- v_cache: bfloat16 [128, 1024, 1, 256], P(('rep', 'dp'), 'sp')
- write_pos: int32 [128], P(('rep', 'dp'))
- valid_len: int32 [128], P(('rep', 'dp'))
Outputs:
- output 1: bfloat16 [128, 4096], P(('rep', 'dp'))
- output 2: bfloat16 [128, 1024, 1, 256], P(('rep', 'dp'), 'sp')
- output 3: bfloat16 [128, 1024, 1, 256], P(('rep', 'dp'), 'sp')
All inputs are finite; a program needn't handle non-finite values.
Results may differ from the reference program's by a relative error of at most 0.00657726.
Values are sent between devices in bfloat16 or wider.
A program may use at most 1 GiB of HBM per device.

```python
import jax
import jax.numpy as jnp
from jax import lax

MODEL_DIM = 4096
NUM_HEADS = 16
KV_HEADS = 1
HEAD_DIM = 256
BATCH_SIZE = 128
CACHE_LEN = 1024
SEGMENTS = 16


def draw_lengths(rng_key):
    keys = jax.random.split(rng_key, 3)
    shortest = CACHE_LEN // 4
    write_pos = jax.random.randint(keys[0], (BATCH_SIZE,), shortest - 1, CACHE_LEN, jnp.int32)
    long_row = jax.random.randint(keys[1], (), 0, BATCH_SIZE, jnp.int32)
    short_row = (long_row + 1 + jax.random.randint(keys[2], (), 0, BATCH_SIZE - 1, jnp.int32)) % BATCH_SIZE
    row_ids = jnp.arange(BATCH_SIZE, dtype=jnp.int32)
    write_pos = jnp.where(row_ids == long_row, CACHE_LEN - 1, write_pos)
    write_pos = jnp.where(row_ids == short_row, shortest - 1, write_pos)
    return write_pos, write_pos + 1


def setup_inputs(seed: int = 0, part: int = 0) -> dict:
    root = jax.random.key(seed)
    shared = jax.random.split(root, 4)
    own = jax.random.split(jax.random.fold_in(root, part), 8)
    seg_len = CACHE_LEN // SEGMENTS
    proj_width = NUM_HEADS * HEAD_DIM
    kv_width = KV_HEADS * HEAD_DIM
    w_query = (jax.random.normal(shared[0], (MODEL_DIM, proj_width), jnp.float32) * MODEL_DIM ** -0.5).astype(jnp.bfloat16)
    w_key = (jax.random.normal(shared[1], (MODEL_DIM, kv_width), jnp.float32) * MODEL_DIM ** -0.5).astype(jnp.bfloat16)
    w_value = (jax.random.normal(shared[2], (MODEL_DIM, kv_width), jnp.float32) * MODEL_DIM ** -0.5).astype(jnp.bfloat16)
    w_out = (jax.random.normal(shared[3], (proj_width, MODEL_DIM), jnp.float32) * proj_width ** -0.5).astype(jnp.bfloat16)
    hidden = jax.random.normal(own[0], (BATCH_SIZE, MODEL_DIM), jnp.float32).astype(jnp.bfloat16)
    cache_shape = (BATCH_SIZE, SEGMENTS, seg_len, KV_HEADS, HEAD_DIM)
    seg_shape = (BATCH_SIZE, SEGMENTS, 1, KV_HEADS, HEAD_DIM)
    flat_shape = (BATCH_SIZE, CACHE_LEN, KV_HEADS, HEAD_DIM)
    k_cache = (jax.random.normal(own[1], cache_shape, jnp.float32) + jax.random.normal(own[2], seg_shape, jnp.float32)).reshape(flat_shape).astype(jnp.bfloat16)
    v_cache = (jax.random.normal(own[3], cache_shape, jnp.float32) + jax.random.normal(own[4], seg_shape, jnp.float32)).reshape(flat_shape).astype(jnp.bfloat16)
    write_pos, valid_len = draw_lengths(own[5])
    return {'hidden': hidden, 'w_query': w_query, 'w_key': w_key, 'w_value': w_value, 'w_out': w_out, 'k_cache': k_cache, 'v_cache': v_cache, 'write_pos': write_pos, 'valid_len': valid_len}


def reference(hidden, w_query, w_key, w_value, w_out, k_cache, v_cache, write_pos, valid_len):
    group_size = NUM_HEADS // KV_HEADS
    query = jnp.dot(hidden, w_query, preferred_element_type=jnp.float32).astype(jnp.bfloat16)
    query = query.reshape(BATCH_SIZE, KV_HEADS, group_size, HEAD_DIM)
    key_new = jnp.dot(hidden, w_key, preferred_element_type=jnp.float32).astype(jnp.bfloat16)
    value_new = jnp.dot(hidden, w_value, preferred_element_type=jnp.float32).astype(jnp.bfloat16)
    positions = jnp.arange(CACHE_LEN, dtype=jnp.int32)
    at_pos = (positions[None, :] == write_pos[:, None])[:, :, None, None]
    k_next = jnp.where(at_pos, key_new.reshape(BATCH_SIZE, 1, KV_HEADS, HEAD_DIM), k_cache)
    v_next = jnp.where(at_pos, value_new.reshape(BATCH_SIZE, 1, KV_HEADS, HEAD_DIM), v_cache)

    def one_row(row_args):
        q_row, k_row, v_row, length = row_args
        scores = jnp.einsum('kgd,skd->kgs', q_row.astype(jnp.float32), k_row.astype(jnp.float32)) * HEAD_DIM ** -0.5
        scores = jnp.where(positions < length, scores, -jnp.inf)
        row_max = jnp.max(scores, axis=-1, keepdims=True)
        weights = jnp.exp(scores - row_max)
        total = jnp.sum(weights, axis=-1, keepdims=True)
        return jnp.einsum('kgs,skd->kgd', weights, v_row.astype(jnp.float32)) / total

    attention = lax.map(one_row, (query, k_next, v_next, valid_len))
    attention = attention.reshape(BATCH_SIZE, NUM_HEADS * HEAD_DIM).astype(jnp.bfloat16)
    attn_out = jnp.dot(attention, w_out, preferred_element_type=jnp.float32).astype(jnp.bfloat16)
    return (attn_out, k_next, v_next)
```

```python
import jax
import jax.numpy as jnp
from jax import lax
from jax.experimental import pallas as pl
from jax.experimental.pallas import tpu as pltpu
from jax.sharding import PartitionSpec as P

MESH = pl.DeviceIdType.MESH
F32, BF16 = jnp.float32, jnp.bfloat16
LOWEST = float(jnp.finfo(jnp.float32).min)

ROWS = 64
SEQ = 256
DIM = 4096
HD = 256
HEADS = 16
GROUP = 8
CHUNK = 16
NCH = ROWS // CHUNK
NPAIR = CHUNK // 2
CR = NPAIR * 8
HALF = 32
BLK = 1024
NW = 9


def step_kernel(hid_hbm, wq_hbm, wk_hbm, wv_hbm, wo_hbm, kc_hbm, vc_hbm, wp_hbm, vl_hbm,
                out_ref, k_ref, v_ref,
                hid, wbuf, wo, wp, vl, qf, kvn, qsend, qrecv, rowid,
                acc, ml, racc1, rml1, racc2, rml2, osum, obf,
                pd, px, pk, rd, rx, fin,
                s_in, s_w, s_k, s_v, s_wo,
                qs, qr, a1s, a1r, m1s, m1r, a2s, a2r, m2s, m2r,
                rds, rdr, rxs, rxr, gxs, gxr, gds, gdr, grs, grr):
    sp = lax.axis_index('sp')
    x, c = sp // 2, sp % 2
    sib = 2 * x + (1 - c)
    xp = 2 * (1 - x) + c
    first_pos = sp * SEQ

    def remote(src, dst, ss, rs, peer):
        return pltpu.make_async_remote_copy(src_ref=src, dst_ref=dst, send_sem=ss, recv_sem=rs,
                                            device_id={'sp': peer}, device_id_type=MESH)

    hid_cp = pltpu.make_async_copy(hid_hbm, hid, s_in.at[0])
    wp_cp = pltpu.make_async_copy(wp_hbm, wp, s_in.at[1])
    vl_cp = pltpu.make_async_copy(vl_hbm, vl, s_in.at[2])
    hid_cp.start()

    def wq_cp(i):
        cols = pl.ds(pl.multiple_of((8 * c + i) * HD, HD), HD)
        return pltpu.make_async_copy(wq_hbm.at[:, cols], wbuf.at[i], s_w.at[i])

    def k_cp(g):
        rows = pl.ds(g * GROUP * SEQ, GROUP * SEQ)
        return pltpu.make_async_copy(kc_hbm.at[rows], k_ref.at[rows], s_k.at[g])

    def v_cp(g):
        rows = pl.ds(g * GROUP * SEQ, GROUP * SEQ)
        return pltpu.make_async_copy(vc_hbm.at[rows], v_ref.at[rows], s_v.at[g])

    def wo_cp(i):
        rows = pl.ds(i * 256, 256)
        return pltpu.make_async_copy(wo_hbm.at[rows], wo.at[rows], s_wo.at[i])

    def start_w(i, _):
        wq_cp(i).start()
        return 0

    lax.fori_loop(0, 8, start_w, 0)

    @pl.when(c == 0)
    def _():
        pltpu.make_async_copy(wk_hbm, wbuf.at[8], s_w.at[8]).start()

    @pl.when(c == 1)
    def _():
        pltpu.make_async_copy(wv_hbm, wbuf.at[8], s_w.at[8]).start()

    wp_cp.start()
    vl_cp.start()

    barrier = pltpu.get_barrier_semaphore()
    for peer in (sib, xp):
        pl.semaphore_signal(barrier, inc=1, device_id={'sp': peer}, device_id_type=MESH)

    rowid[...] = lax.broadcasted_iota(jnp.int32, (SEQ, HD), 0).astype(F32).astype(BF16)
    hid_cp.wait()
    pl.semaphore_wait(barrier, 2)

    def spread(slot, q):
        for h in range(2):
            qf[h, pl.ds(slot, ROWS, stride=HEADS), :] = q[:, h * 128:(h + 1) * 128]

    def project(i):
        pltpu.make_async_copy(wk_hbm, wbuf.at[i], s_w.at[i]).wait()
        res = jnp.dot(hid[...], wbuf[i], preferred_element_type=F32).astype(BF16)
        qsend[i] = res
        remote(qsend.at[i], qrecv.at[i], qs.at[i], qr.at[i], sib).start()
        return res.astype(F32)

    def head_step(i, _):
        res = project(i)
        slot = 8 * (i // 4) + 4 * c + i % 4
        spread(slot, res)
        k_cp(i).start()
        v_cp(i).start()
        return 0

    lax.fori_loop(0, 8, head_step, 0)
    kvn[c] = project(8)
    for i in range(4):
        wo_cp(i).start()

    def q_desc(i):
        return remote(qsend.at[i], qrecv.at[i], qs.at[i], qr.at[i], sib)

    def take_head(i, _):
        q_desc(i).wait_recv()
        slot = 8 * (i // 4) + 4 * (1 - c) + i % 4
        spread(slot, qrecv[i].astype(F32))
        return 0

    lax.fori_loop(0, 8, take_head, 0)
    q_desc(8).wait_recv()
    kvn[1 - c] = qrecv[8].astype(F32)
    wp_cp.wait()
    vl_cp.wait()

    sub = lax.broadcasted_iota(jnp.int32, (8, HD), 0)
    sub1 = lax.broadcasted_iota(jnp.int32, (8, 128), 0)
    lane1 = lax.broadcasted_iota(jnp.int32, (8, 128), 1)
    lane = lax.broadcasted_iota(jnp.int32, (HEADS, SEQ), 1)

    def insert(ref, b, new):
        rows = pl.ds(pl.multiple_of(b * SEQ, SEQ), SEQ)
        old = ref[rows, :]
        pos = jnp.full((16, HD), (wp[b] - first_pos).astype(F32), F32).astype(BF16)
        row16 = jnp.broadcast_to(new[pl.ds(b, 1), :], (16, HD)).astype(BF16)
        parts = []
        for r in range(SEQ // 16):
            hit = rowid[r * 16:(r + 1) * 16, :] == pos
            parts.append(jnp.where(hit, row16, old[r * 16:(r + 1) * 16, :]))
        both = jnp.concatenate(parts, axis=0)
        ref[rows, :] = both
        return both

    def attend(b):
        kb = insert(k_ref, b, kvn.at[0])
        vb = insert(v_ref, b, kvn.at[1])
        rows = pl.ds(pl.multiple_of(b * HEADS, HEADS), HEADS)
        q = jnp.concatenate([qf[0, rows, :], qf[1, rows, :]], axis=1).astype(BF16)
        s = lax.dot_general(q, kb, (((1,), (1,)), ((), ())), preferred_element_type=F32) * (HD ** -0.5)
        s = jnp.where(lane < vl[b] - first_pos, s, -jnp.inf)
        m = jnp.maximum(jnp.max(s, axis=1, keepdims=True), LOWEST)
        p = jnp.exp(s - m)
        l = jnp.sum(p, axis=1, keepdims=True)
        o = jnp.dot(p.astype(BF16), vb, preferred_element_type=F32)
        return o, jnp.broadcast_to(m, (HEADS, 128)), jnp.broadcast_to(l, (HEADS, 128))

    def pack(t0, t1, low):
        return (jnp.where(low, t0, pltpu.roll(t1, 4, 0)), jnp.where(low, pltpu.roll(t0, 4, 0), t1))

    def chunk_attention(ch):
        def group(g2, tiles):
            g = 2 * ch + g2
            k_cp(g).wait()
            v_cp(g).wait()
            tiles = list(tiles)
            res = [attend(g * GROUP + j) for j in range(GROUP)]
            for jp in range(GROUP // 2):
                (o0, m0, l0), (o1, m1, l1) = res[2 * jp], res[2 * jp + 1]
                p = g2 * (GROUP // 2) + jp
                for core in range(2):
                    r = slice(8 * core, 8 * core + 8)
                    os = pack(o0[r], o1[r], sub < 4)
                    ms = pack(m0[r], m1[r], sub1 < 4)
                    ls = pack(l0[r], l1[r], sub1 < 4)
                    for xd in range(2):
                        acc[core, ch, xd, pl.ds(pl.multiple_of(p * 8, 8), 8), :] = os[xd]
                        t = tiles[2 * core + xd]
                        t = jnp.where(lane1 == p, ms[xd], t)
                        tiles[2 * core + xd] = jnp.where(lane1 == p + 64, ls[xd], t)
            return tuple(tiles)

        zero = jnp.zeros((8, 128), F32)
        tiles = lax.fori_loop(0, 2, group, (zero,) * 4)
        for core in range(2):
            for xd in range(2):
                ml[core, ch, xd] = tiles[2 * core + xd]

    def d2d(ch):
        return (remote(acc.at[1 - c, ch], racc1.at[ch], a1s.at[ch], a1r.at[ch], sib),
                remote(ml.at[1 - c, ch], rml1.at[ch], m1s.at[ch], m1r.at[ch], sib))

    def xlink(ch):
        return (remote(acc.at[c, ch, 1 - x], racc2.at[ch], a2s.at[ch], a2r.at[ch], xp),
                remote(ml.at[c, ch, 1 - x], rml2.at[ch], m2s.at[ch], m2r.at[ch], xp))

    def scales(mla, mlb):
        top = jnp.maximum(mla, mlb)
        sa, sb = jnp.exp(mla - top), jnp.exp(mlb - top)
        total = mla * pltpu.roll(sa, 64, 1) + mlb * pltpu.roll(sb, 64, 1)
        return top, sa, sb, total

    def merge_core(ch):
        for desc in d2d(ch):
            desc.wait_recv()
        for xd in range(2):
            top, sa, sb, total = scales(ml[c, ch, xd], rml1[ch, xd])
            ml[c, ch, xd] = jnp.where(lane1 < 64, top, total)
            for p in range(NPAIR):
                r = slice(p * 8, p * 8 + 8)
                acc[c, ch, xd, r, :] = (acc[c, ch, xd, r, :] * sa[:, p:p + 1]
                                        + racc1[ch, xd, r, :] * sb[:, p:p + 1])
        for desc in xlink(ch):
            desc.start()

    def merge_chip(ch):
        for desc in xlink(ch):
            desc.wait_recv()
        top, sa, sb, total = scales(ml[c, ch, x], rml2[ch])
        inv = pltpu.roll(1.0 / jnp.where(lane1 < 64, 1.0, total), 64, 1)
        sa, sb = sa * inv, sb * inv
        for p in range(NPAIR):
            r = slice(p * 8, p * 8 + 8)
            o = acc[c, ch, x, r, :] * sa[:, p:p + 1] + racc2[ch, r, :] * sb[:, p:p + 1]
            for h in range(2):
                osum[h, pl.ds(pl.multiple_of(ch * CR + p * 8, 8), 8), :] = o[:, h * 128:(h + 1) * 128]

    def core_sum(hf, xd):
        return remote(pd.at[hf, xd], rd.at[hf, xd], rds.at[2 * hf + xd], rdr.at[2 * hf + xd], sib)

    def chip_sum(hf):
        return remote(px.at[hf], rx.at[hf], rxs.at[hf], rxr.at[hf], xp)

    def project_out(hf):
        rows = pl.ds(hf * HALF, HALF)
        for r in range(4):
            for h in range(2):
                lanes = slice(r * HD + h * 128, r * HD + (h + 1) * 128)
                obf[rows, lanes] = osum[h, pl.ds(hf * 4 * HALF + r, HALF, stride=4), :].astype(BF16)

        def block(dst, j):
            def piece(n, _):
                cols = pl.ds(pl.multiple_of(j * BLK + n * 512, 512), 512)
                dst[:, pl.ds(pl.multiple_of(n * 512, 512), 512)] = jnp.dot(
                    obf[rows, :], wo[:, cols], preferred_element_type=F32)
                return 0
            lax.fori_loop(0, BLK // 512, piece, 0)

        block(pd.at[hf, 0], 2 * (1 - x) + 1 - c)
        core_sum(hf, 0).start()
        block(px.at[hf], 2 * (1 - x) + c)
        core_sum(hf, 0).wait_recv()
        px[hf] = px[hf] + rd[hf, 0]
        chip_sum(hf).start()
        block(pd.at[hf, 1], 2 * x + 1 - c)
        core_sum(hf, 1).start()
        block(pk.at[hf], 2 * x + c)

    def own(hf, j):
        return fin.at[j, pl.ds(hf * HALF, HALF)]

    def gather_x(hf):
        return remote(own(hf, sp), own(hf, sp), gxs.at[hf], gxr.at[hf], xp)

    def gather_d(hf):
        return remote(own(hf, sp), own(hf, sp), gds.at[hf], gdr.at[hf], sib)

    def gather_r(hf):
        return remote(own(hf, xp), own(hf, xp), grs.at[hf], grr.at[hf], sib)

    def finish(hf):
        core_sum(hf, 1).wait_recv()
        chip_sum(hf).wait_recv()
        fin[sp, pl.ds(hf * HALF, HALF), :] = ((pk[hf] + rd[hf, 1]) + rx[hf]).astype(BF16)
        gather_x(hf).start()
        gather_d(hf).start()

    def relay(hf):
        remote(own(hf, sp), own(hf, xp), gxs.at[hf], gxr.at[hf], xp).wait_recv()
        gather_r(hf).start()

    def pipeline(ch, _):
        @pl.when(ch < NCH)
        def _():
            chunk_attention(ch)
            for desc in d2d(ch):
                desc.start()

        @pl.when(ch >= 1)
        def _():
            merge_core(ch - 1)
        return 0

    lax.fori_loop(0, NCH + 1, pipeline, 0)

    def chips(ch, _):
        merge_chip(ch)
        return 0

    lax.fori_loop(0, 2, chips, 0)
    for i in range(4):
        wo_cp(i).wait()
    project_out(0)
    lax.fori_loop(2, NCH, chips, 0)
    project_out(1)
    finish(0)
    relay(0)
    finish(1)
    relay(1)

    for hf in range(2):
        gather_d(hf).wait_recv()
        gather_r(hf).wait_recv()
    for j in range(4):
        out_ref[:, j * BLK:(j + 1) * BLK] = fin[j]

    def end_q(i, _):
        q_desc(i).wait_send()
        return 0

    lax.fori_loop(0, NW, end_q, 0)

    def end_chunk(ch, _):
        for desc in d2d(ch) + xlink(ch):
            desc.wait_send()
        return 0

    lax.fori_loop(0, NCH, end_chunk, 0)
    for hf in range(2):
        core_sum(hf, 0).wait_send()
        core_sum(hf, 1).wait_send()
        chip_sum(hf).wait_send()
        gather_x(hf).wait_send()
        gather_d(hf).wait_send()
        gather_r(hf).wait_send()


def solution(mesh):
    row_spec = P(('rep', 'dp'), None)
    cache_spec = P(('rep', 'dp'), 'sp', None, None)
    len_spec = P(('rep', 'dp'))

    def local_step(hidden, w_query, w_key, w_value, w_out, k_cache, v_cache, write_pos, valid_len):
        flat = (ROWS * SEQ, HD)
        args = (hidden, w_query, w_key, w_value, w_out, k_cache.reshape(flat), v_cache.reshape(flat),
                write_pos, valid_len)
        args = tuple(pltpu.with_memory_space_constraint(a, pltpu.HBM) for a in args)
        vm = pl.BlockSpec(memory_space=pltpu.VMEM)
        dma = pltpu.SemaphoreType.DMA
        out, k_new, v_new = pl.pallas_call(
            step_kernel,
            out_shape=[pltpu.VMEM((ROWS, DIM), BF16), pltpu.VMEM(flat, BF16), pltpu.VMEM(flat, BF16)],
            in_specs=[pl.BlockSpec(memory_space=pltpu.HBM)] * 9,
            out_specs=[vm, vm, vm],
            scratch_shapes=[
                pltpu.VMEM((ROWS, DIM), BF16),
                pltpu.VMEM((NW, DIM, HD), BF16),
                pltpu.VMEM((BLK, DIM), BF16),
                pltpu.SMEM((ROWS,), jnp.int32),
                pltpu.SMEM((ROWS,), jnp.int32),
                pltpu.VMEM((2, ROWS * HEADS, 128), F32),
                pltpu.VMEM((2, ROWS, HD), F32),
                pltpu.VMEM((NW, ROWS, HD), BF16),
                pltpu.VMEM((NW, ROWS, HD), BF16),
                pltpu.VMEM((SEQ, HD), BF16),
                pltpu.VMEM((2, NCH, 2, CR, HD), F32),
                pltpu.VMEM((2, NCH, 2, 8, 128), F32),
                pltpu.VMEM((NCH, 2, CR, HD), F32),
                pltpu.VMEM((NCH, 2, 8, 128), F32),
                pltpu.VMEM((NCH, CR, HD), F32),
                pltpu.VMEM((NCH, 8, 128), F32),
                pltpu.VMEM((2, 4 * ROWS, 128), F32),
                pltpu.VMEM((ROWS, BLK), BF16),
                pltpu.VMEM((2, 2, HALF, BLK), F32),
                pltpu.VMEM((2, HALF, BLK), F32),
                pltpu.VMEM((2, HALF, BLK), F32),
                pltpu.VMEM((2, 2, HALF, BLK), F32),
                pltpu.VMEM((2, HALF, BLK), F32),
                pltpu.VMEM((4, ROWS, BLK), BF16),
                dma((3,)), dma((NW,)), dma((8,)), dma((8,)), dma((4,)),
                dma((NW,)), dma((NW,)),
                dma((NCH,)), dma((NCH,)), dma((NCH,)), dma((NCH,)),
                dma((NCH,)), dma((NCH,)), dma((NCH,)), dma((NCH,)),
                dma((4,)), dma((4,)), dma((2,)), dma((2,)),
                dma((2,)), dma((2,)), dma((2,)), dma((2,)), dma((2,)), dma((2,)),
            ],
            compiler_params=pltpu.CompilerParams(
                vmem_limit_bytes=44 * 2 ** 20, collective_id=0, has_side_effects=True),
            name='decode_step',
        )(*args)
        return out, k_new.reshape(k_cache.shape), v_new.reshape(v_cache.shape)

    return jax.shard_map(local_step, mesh=mesh, in_specs=(row_spec, P(), P(), P(), P('sp', None), cache_spec, cache_spec, len_spec, len_spec), out_specs=(row_spec, cache_spec, cache_spec), check_vma=False)
```

```python
import jax
import jax.numpy as jnp
from jax import lax
from jax.experimental import pallas as pl
from jax.experimental.pallas import tpu as pltpu
from jax.sharding import PartitionSpec as P

MESH = pl.DeviceIdType.MESH
F32, BF16 = jnp.float32, jnp.bfloat16
LOWEST = float(jnp.finfo(jnp.float32).min)

ROWS = 64
SEQ = 256
DIM = 4096
HD = 256
HEADS = 16
GROUP = 8
CHUNK = 16
NCH = ROWS // CHUNK
NPAIR = CHUNK // 2
CR = NPAIR * 8
HALF = 32
BLK = 1024
NW = 9


def step_kernel(hid_hbm, wq_hbm, wk_hbm, wv_hbm, wo_hbm, kc_hbm, vc_hbm, wp_hbm, vl_hbm,
                out_ref, k_ref, v_ref, kvn,
                hid, wbuf, wo, wp, vl, qf, qsend, qrecv, prob, pnew,
                acc, ml, racc1, rml1, racc2, rml2, osum, obf,
                pd, px, pk, rd, rx, fin,
                s_in, s_w, s_k, s_v, s_wo,
                qs, qr, a1s, a1r, m1s, m1r, a2s, a2r, m2s, m2r,
                rds, rdr, rxs, rxr, gxs, gxr, gds, gdr, grs, grr):
    sp = lax.axis_index('sp')
    x, c = sp // 2, sp % 2
    sib = 2 * x + (1 - c)
    xp = 2 * (1 - x) + c
    first_pos = sp * SEQ

    def remote(src, dst, ss, rs, peer):
        return pltpu.make_async_remote_copy(src_ref=src, dst_ref=dst, send_sem=ss, recv_sem=rs,
                                            device_id={'sp': peer}, device_id_type=MESH)

    hid_cp = pltpu.make_async_copy(hid_hbm, hid, s_in.at[0])
    wp_cp = pltpu.make_async_copy(wp_hbm, wp, s_in.at[1])
    vl_cp = pltpu.make_async_copy(vl_hbm, vl, s_in.at[2])
    hid_cp.start()

    def wq_cp(i):
        cols = pl.ds(pl.multiple_of((8 * c + i) * HD, HD), HD)
        return pltpu.make_async_copy(wq_hbm.at[:, cols], wbuf.at[i], s_w.at[i])

    def k_cp(g):
        rows = pl.ds(g * GROUP * SEQ, GROUP * SEQ)
        return pltpu.make_async_copy(kc_hbm.at[rows], k_ref.at[rows], s_k.at[g])

    def v_cp(g):
        rows = pl.ds(g * GROUP * SEQ, GROUP * SEQ)
        return pltpu.make_async_copy(vc_hbm.at[rows], v_ref.at[rows], s_v.at[g])

    def wo_cp(i):
        rows = pl.ds(i * 256, 256)
        return pltpu.make_async_copy(wo_hbm.at[rows], wo.at[rows], s_wo.at[i])

    def start_w(i, _):
        wq_cp(i).start()
        return 0

    lax.fori_loop(0, 8, start_w, 0)

    @pl.when(c == 0)
    def _():
        pltpu.make_async_copy(wk_hbm, wbuf.at[8], s_w.at[8]).start()

    @pl.when(c == 1)
    def _():
        pltpu.make_async_copy(wv_hbm, wbuf.at[8], s_w.at[8]).start()

    wp_cp.start()
    vl_cp.start()

    barrier = pltpu.get_barrier_semaphore()
    for peer in (sib, xp):
        pl.semaphore_signal(barrier, inc=1, device_id={'sp': peer}, device_id_type=MESH)

    hid_cp.wait()
    pl.semaphore_wait(barrier, 2)

    def spread(slot, q):
        for h in range(2):
            qf[h, pl.ds(slot, ROWS, stride=HEADS), :] = q[:, h * 128:(h + 1) * 128]

    def project(i):
        pltpu.make_async_copy(wk_hbm, wbuf.at[i], s_w.at[i]).wait()
        res = jnp.dot(hid[...], wbuf[i], preferred_element_type=F32).astype(BF16)
        qsend[i] = res
        remote(qsend.at[i], qrecv.at[i], qs.at[i], qr.at[i], sib).start()
        return res.astype(F32)

    def head_step(i, _):
        res = project(i)
        slot = 8 * (i // 4) + 4 * c + i % 4
        spread(slot, res)
        k_cp(i).start()
        v_cp(i).start()
        return 0

    lax.fori_loop(0, 8, head_step, 0)
    kvn[c] = project(8)
    for i in range(4):
        wo_cp(i).start()

    def q_desc(i):
        return remote(qsend.at[i], qrecv.at[i], qs.at[i], qr.at[i], sib)

    def take_head(i, _):
        q_desc(i).wait_recv()
        slot = 8 * (i // 4) + 4 * (1 - c) + i % 4
        spread(slot, qrecv[i].astype(F32))
        return 0

    lax.fori_loop(0, 8, take_head, 0)
    q_desc(8).wait_recv()
    kvn[1 - c] = qrecv[8].astype(F32)
    wp_cp.wait()
    vl_cp.wait()

    sub = lax.broadcasted_iota(jnp.int32, (8, HD), 0)
    sub1 = lax.broadcasted_iota(jnp.int32, (8, 128), 0)
    lane1 = lax.broadcasted_iota(jnp.int32, (8, 128), 1)
    lane = lax.broadcasted_iota(jnp.int32, (HEADS, SEQ), 1)

    def cache_rows(b):
        return pl.ds(pl.multiple_of(b * SEQ, SEQ), SEQ)

    def weigh(b, j):
        rows = pl.ds(pl.multiple_of(b * HEADS, HEADS), HEADS)
        q = jnp.concatenate([qf[0, rows, :], qf[1, rows, :]], axis=1)
        s = lax.dot_general(q.astype(BF16), k_ref[cache_rows(b), :], (((1,), (1,)), ((), ())),
                            preferred_element_type=F32)
        s_new = jnp.sum(q * kvn[0, pl.ds(b, 1), :], axis=1, keepdims=True)
        here = lane == wp[b] - first_pos
        s = jnp.where(here, s_new, s) * (HD ** -0.5)
        s = jnp.where(lane < vl[b] - first_pos, s, -jnp.inf)
        m = jnp.maximum(jnp.max(s, axis=1, keepdims=True), LOWEST)
        p = jnp.exp(s - m)
        l = jnp.sum(p, axis=1, keepdims=True)
        p_new = jnp.sum(jnp.where(here, p, 0.0), axis=1, keepdims=True)
        mine = slice(j * HEADS, (j + 1) * HEADS)
        prob[mine, :] = jnp.where(here, 0.0, p).astype(BF16)
        pnew[mine, :] = jnp.broadcast_to(p_new, (HEADS, 128))
        return jnp.broadcast_to(m, (HEADS, 128)), jnp.broadcast_to(l, (HEADS, 128))

    def value_sum(b, j):
        mine = slice(j * HEADS, (j + 1) * HEADS)
        o = jnp.dot(prob[mine, :], v_ref[cache_rows(b), :], preferred_element_type=F32)
        p_new = pnew[mine, :]
        return o + jnp.concatenate([p_new, p_new], axis=1) * kvn[1, pl.ds(b, 1), :]

    def pack(t0, t1, low):
        return (jnp.where(low, t0, pltpu.roll(t1, 4, 0)), jnp.where(low, pltpu.roll(t0, 4, 0), t1))

    def chunk_attention(ch):
        for g2 in range(CHUNK // GROUP):
            k_cp(ch * (CHUNK // GROUP) + g2).wait()

        @pl.when(ch >= 0)
        def _():
            tiles = [jnp.zeros((8, 128), F32)] * 4
            for p in range(NPAIR):
                m0, l0 = weigh(ch * CHUNK + 2 * p, 2 * p)
                m1, l1 = weigh(ch * CHUNK + 2 * p + 1, 2 * p + 1)
                for core in range(2):
                    r = slice(8 * core, 8 * core + 8)
                    ms = pack(m0[r], m1[r], sub1 < 4)
                    ls = pack(l0[r], l1[r], sub1 < 4)
                    for xd in range(2):
                        t = jnp.where(lane1 == p, ms[xd], tiles[2 * core + xd])
                        tiles[2 * core + xd] = jnp.where(lane1 == p + 64, ls[xd], t)
            for core in range(2):
                for xd in range(2):
                    ml[core, ch, xd] = tiles[2 * core + xd]

        for g2 in range(CHUNK // GROUP):
            v_cp(ch * (CHUNK // GROUP) + g2).wait()

        @pl.when(ch >= 0)
        def _():
            for p in range(NPAIR):
                o0 = value_sum(ch * CHUNK + 2 * p, 2 * p)
                o1 = value_sum(ch * CHUNK + 2 * p + 1, 2 * p + 1)
                for core in range(2):
                    r = slice(8 * core, 8 * core + 8)
                    os = pack(o0[r], o1[r], sub < 4)
                    for xd in range(2):
                        acc[core, ch, xd, p * 8:p * 8 + 8, :] = os[xd]

    def d2d(ch):
        return (remote(acc.at[1 - c, ch], racc1.at[ch], a1s.at[ch], a1r.at[ch], sib),
                remote(ml.at[1 - c, ch], rml1.at[ch], m1s.at[ch], m1r.at[ch], sib))

    def xlink(ch):
        return (remote(acc.at[c, ch, 1 - x], racc2.at[ch], a2s.at[ch], a2r.at[ch], xp),
                remote(ml.at[c, ch, 1 - x], rml2.at[ch], m2s.at[ch], m2r.at[ch], xp))

    def scales(mla, mlb):
        top = jnp.maximum(mla, mlb)
        sa, sb = jnp.exp(mla - top), jnp.exp(mlb - top)
        total = mla * pltpu.roll(sa, 64, 1) + mlb * pltpu.roll(sb, 64, 1)
        return top, sa, sb, total

    def merge_core(ch):
        for desc in d2d(ch):
            desc.wait_recv()
        for xd in range(2):
            top, sa, sb, total = scales(ml[c, ch, xd], rml1[ch, xd])
            ml[c, ch, xd] = jnp.where(lane1 < 64, top, total)
            for p in range(NPAIR):
                r = slice(p * 8, p * 8 + 8)
                acc[c, ch, xd, r, :] = (acc[c, ch, xd, r, :] * sa[:, p:p + 1]
                                        + racc1[ch, xd, r, :] * sb[:, p:p + 1])
        for desc in xlink(ch):
            desc.start()

    def merge_chip(ch):
        for desc in xlink(ch):
            desc.wait_recv()
        top, sa, sb, total = scales(ml[c, ch, x], rml2[ch])
        inv = pltpu.roll(1.0 / jnp.where(lane1 < 64, 1.0, total), 64, 1)
        sa, sb = sa * inv, sb * inv
        for p in range(NPAIR):
            r = slice(p * 8, p * 8 + 8)
            o = acc[c, ch, x, r, :] * sa[:, p:p + 1] + racc2[ch, r, :] * sb[:, p:p + 1]
            for h in range(2):
                osum[h, pl.ds(pl.multiple_of(ch * CR + p * 8, 8), 8), :] = o[:, h * 128:(h + 1) * 128]

    def core_sum(hf, xd):
        return remote(pd.at[hf, xd], rd.at[hf, xd], rds.at[2 * hf + xd], rdr.at[2 * hf + xd], sib)

    def chip_sum(hf):
        return remote(px.at[hf], rx.at[hf], rxs.at[hf], rxr.at[hf], xp)

    def project_out(hf):
        rows = pl.ds(hf * HALF, HALF)
        for r in range(4):
            for h in range(2):
                lanes = slice(r * HD + h * 128, r * HD + (h + 1) * 128)
                obf[rows, lanes] = osum[h, pl.ds(hf * 4 * HALF + r, HALF, stride=4), :].astype(BF16)

        def block(dst, j):
            def piece(n, _):
                cols = pl.ds(pl.multiple_of(j * BLK + n * 512, 512), 512)
                dst[:, pl.ds(pl.multiple_of(n * 512, 512), 512)] = jnp.dot(
                    obf[rows, :], wo[:, cols], preferred_element_type=F32)
                return 0
            lax.fori_loop(0, BLK // 512, piece, 0)

        block(pd.at[hf, 0], 2 * (1 - x) + 1 - c)
        core_sum(hf, 0).start()
        block(px.at[hf], 2 * (1 - x) + c)
        core_sum(hf, 0).wait_recv()
        px[hf] = px[hf] + rd[hf, 0]
        chip_sum(hf).start()
        block(pd.at[hf, 1], 2 * x + 1 - c)
        core_sum(hf, 1).start()
        block(pk.at[hf], 2 * x + c)

    def own(hf, j):
        return fin.at[j, pl.ds(hf * HALF, HALF)]

    def gather_x(hf):
        return remote(own(hf, sp), own(hf, sp), gxs.at[hf], gxr.at[hf], xp)

    def gather_d(hf):
        return remote(own(hf, sp), own(hf, sp), gds.at[hf], gdr.at[hf], sib)

    def gather_r(hf):
        return remote(own(hf, xp), own(hf, xp), grs.at[hf], grr.at[hf], sib)

    def finish(hf):
        core_sum(hf, 1).wait_recv()
        chip_sum(hf).wait_recv()
        fin[sp, pl.ds(hf * HALF, HALF), :] = ((pk[hf] + rd[hf, 1]) + rx[hf]).astype(BF16)
        gather_x(hf).start()
        gather_d(hf).start()

    def relay(hf):
        remote(own(hf, sp), own(hf, xp), gxs.at[hf], gxr.at[hf], xp).wait_recv()
        gather_r(hf).start()

    def pipeline(ch, _):
        @pl.when(ch < NCH)
        def _():
            chunk_attention(ch)
            for desc in d2d(ch):
                desc.start()

        @pl.when(ch >= 1)
        def _():
            merge_core(ch - 1)
        return 0

    lax.fori_loop(0, NCH + 1, pipeline, 0)

    def chips(ch, _):
        merge_chip(ch)
        return 0

    lax.fori_loop(0, 2, chips, 0)
    for i in range(4):
        wo_cp(i).wait()
    project_out(0)
    lax.fori_loop(2, NCH, chips, 0)
    project_out(1)
    finish(0)
    relay(0)
    finish(1)
    relay(1)

    for hf in range(2):
        gather_d(hf).wait_recv()
        gather_r(hf).wait_recv()
    for j in range(4):
        out_ref[:, j * BLK:(j + 1) * BLK] = fin[j]

    def end_q(i, _):
        q_desc(i).wait_send()
        return 0

    lax.fori_loop(0, NW, end_q, 0)

    def end_chunk(ch, _):
        for desc in d2d(ch) + xlink(ch):
            desc.wait_send()
        return 0

    lax.fori_loop(0, NCH, end_chunk, 0)
    for hf in range(2):
        core_sum(hf, 0).wait_send()
        core_sum(hf, 1).wait_send()
        chip_sum(hf).wait_send()
        gather_x(hf).wait_send()
        gather_d(hf).wait_send()
        gather_r(hf).wait_send()


def cache_kernel(wp, kvn, k_in, v_in, k_ref, v_ref, k_out, v_out, s_k, s_v):
    first_pos = lax.axis_index('sp') * SEQ
    row = lax.broadcasted_iota(jnp.int32, (16, HD), 0)

    def insert(b, _):
        pos = wp[b] - first_pos
        base = jnp.clip(pos, 0, SEQ - 1) // 16 * 16
        rows = pl.ds(pl.multiple_of(b * SEQ + base, 16), 16)
        hit = row == pos - base
        for ref, i in ((k_ref, 0), (v_ref, 1)):
            ref[rows, :] = jnp.where(hit, kvn[i, pl.ds(b, 1), :], ref[rows, :].astype(F32)).astype(BF16)
        return 0

    lax.fori_loop(0, ROWS, insert, 0, unroll=8)

    def copies(g):
        rows = pl.ds(g * GROUP * SEQ, GROUP * SEQ)
        return (pltpu.make_async_copy(k_ref.at[rows], k_out.at[rows], s_k.at[g]),
                pltpu.make_async_copy(v_ref.at[rows], v_out.at[rows], s_v.at[g]))

    for g in range(8):
        for cp in copies(g):
            cp.start()
    for g in range(8):
        for cp in copies(g):
            cp.wait()


def solution(mesh):
    row_spec = P(('rep', 'dp'), None)
    cache_spec = P(('rep', 'dp'), 'sp', None, None)
    len_spec = P(('rep', 'dp'))

    def local_step(hidden, w_query, w_key, w_value, w_out, k_cache, v_cache, write_pos, valid_len):
        flat = (ROWS * SEQ, HD)
        args = (hidden, w_query, w_key, w_value, w_out, k_cache.reshape(flat), v_cache.reshape(flat),
                write_pos, valid_len)
        args = tuple(pltpu.with_memory_space_constraint(a, pltpu.HBM) for a in args)
        vm = pl.BlockSpec(memory_space=pltpu.VMEM)
        dma = pltpu.SemaphoreType.DMA
        out, k_old, v_old, kv_new = pl.pallas_call(
            step_kernel,
            out_shape=[pltpu.VMEM((ROWS, DIM), BF16), pltpu.VMEM(flat, BF16), pltpu.VMEM(flat, BF16),
                       pltpu.VMEM((2, ROWS, HD), F32)],
            in_specs=[pl.BlockSpec(memory_space=pltpu.HBM)] * 9,
            out_specs=[vm, vm, vm, vm],
            scratch_shapes=[
                pltpu.VMEM((ROWS, DIM), BF16),
                pltpu.VMEM((NW, DIM, HD), BF16),
                pltpu.VMEM((BLK, DIM), BF16),
                pltpu.SMEM((ROWS,), jnp.int32),
                pltpu.SMEM((ROWS,), jnp.int32),
                pltpu.VMEM((2, ROWS * HEADS, 128), F32),
                pltpu.VMEM((NW, ROWS, HD), BF16),
                pltpu.VMEM((NW, ROWS, HD), BF16),
                pltpu.VMEM((CHUNK * HEADS, SEQ), BF16),
                pltpu.VMEM((CHUNK * HEADS, 128), F32),
                pltpu.VMEM((2, NCH, 2, CR, HD), F32),
                pltpu.VMEM((2, NCH, 2, 8, 128), F32),
                pltpu.VMEM((NCH, 2, CR, HD), F32),
                pltpu.VMEM((NCH, 2, 8, 128), F32),
                pltpu.VMEM((NCH, CR, HD), F32),
                pltpu.VMEM((NCH, 8, 128), F32),
                pltpu.VMEM((2, 4 * ROWS, 128), F32),
                pltpu.VMEM((ROWS, BLK), BF16),
                pltpu.VMEM((2, 2, HALF, BLK), F32),
                pltpu.VMEM((2, HALF, BLK), F32),
                pltpu.VMEM((2, HALF, BLK), F32),
                pltpu.VMEM((2, 2, HALF, BLK), F32),
                pltpu.VMEM((2, HALF, BLK), F32),
                pltpu.VMEM((4, ROWS, BLK), BF16),
                dma((3,)), dma((NW,)), dma((8,)), dma((8,)), dma((4,)),
                dma((NW,)), dma((NW,)),
                dma((NCH,)), dma((NCH,)), dma((NCH,)), dma((NCH,)),
                dma((NCH,)), dma((NCH,)), dma((NCH,)), dma((NCH,)),
                dma((4,)), dma((4,)), dma((2,)), dma((2,)),
                dma((2,)), dma((2,)), dma((2,)), dma((2,)), dma((2,)), dma((2,)),
            ],
            compiler_params=pltpu.CompilerParams(
                vmem_limit_bytes=44 * 2 ** 20, collective_id=0, has_side_effects=True),
            name='decode_step',
        )(*args)
        anywhere = pl.BlockSpec(memory_space=pltpu.HBM)
        _, _, k_new, v_new = pl.pallas_call(
            cache_kernel,
            out_shape=[pltpu.VMEM(flat, BF16), pltpu.VMEM(flat, BF16),
                       pltpu.HBM(flat, BF16), pltpu.HBM(flat, BF16)],
            in_specs=[pl.BlockSpec(memory_space=pltpu.SMEM), vm, vm, vm],
            out_specs=[vm, vm, anywhere, anywhere],
            scratch_shapes=[dma((8,)), dma((8,))],
            input_output_aliases={2: 0, 3: 1},
            compiler_params=pltpu.CompilerParams(vmem_limit_bytes=2 ** 20),
            name='cache_update',
        )(write_pos, kv_new, k_old, v_old)
        return out, k_new.reshape(k_cache.shape), v_new.reshape(v_cache.shape)

    return jax.shard_map(local_step, mesh=mesh, in_specs=(row_spec, P(), P(), P(), P('sp', None), cache_spec, cache_spec, len_spec, len_spec), out_specs=(row_spec, cache_spec, cache_spec), check_vma=False)
```

```python
import jax
import jax.numpy as jnp
from jax import lax
from jax.experimental import pallas as pl
from jax.experimental.pallas import tpu as pltpu
from jax.sharding import PartitionSpec as P

MESH = pl.DeviceIdType.MESH
F32, BF16 = jnp.float32, jnp.bfloat16
LOWEST = float(jnp.finfo(jnp.float32).min)

ROWS = 64
SEQ = 256
DIM = 4096
HD = 256
HEADS = 16
GROUP = 8
CHUNK = 16
NCH = ROWS // CHUNK
NPAIR = CHUNK // 2
CR = NPAIR * 8
OUT = 16
NOUT = ROWS // OUT
BLK = 1024
AHEAD = 4
SHARED = 2
NOWN = 8 - SHARED
NW = NOWN + 1
DIST = 1


def step_kernel(hid_hbm, wq_hbm, wk_hbm, wv_hbm, wo_hbm, kc_hbm, vc_hbm, wp_hbm, vl_hbm,
                out_ref, k_ref, v_ref, kvn,
                hid, wbuf, wo, wp, vl, qf, qsend, qrecv, qchip, prob, pnew,
                acc, ml, racc1, rml1, racc2, rml2, osum, obf,
                pd, px, pk, rd, rx,
                s_in, s_w, s_k, s_v, s_wo,
                qs, qr, qxs, qxr, a1s, a1r, m1s, m1r, a2s, a2r, m2s, m2r,
                rds, rdr, rxs, rxr):
    sp = lax.axis_index('sp')
    x, c = sp // 2, sp % 2
    sib = 2 * x + (1 - c)
    xp = 2 * (1 - x) + c
    first_pos = sp * SEQ

    def remote(src, dst, ss, rs, peer):
        return pltpu.make_async_remote_copy(src_ref=src, dst_ref=dst, send_sem=ss, recv_sem=rs,
                                            device_id={'sp': peer}, device_id_type=MESH)

    hid_cp = pltpu.make_async_copy(hid_hbm, hid, s_in.at[0])
    wp_cp = pltpu.make_async_copy(wp_hbm, wp, s_in.at[1])
    vl_cp = pltpu.make_async_copy(vl_hbm, vl, s_in.at[2])
    hid_cp.start()

    def head(i, chip):
        return i + chip * (7 - 2 * i)

    def wq_cp(i):
        cols = pl.ds(pl.multiple_of((8 * c + head(i, x)) * HD, HD), HD)
        return pltpu.make_async_copy(wq_hbm.at[:, cols], wbuf.at[i], s_w.at[i])

    def k_cp(g):
        rows = pl.ds(g * GROUP * SEQ, GROUP * SEQ)
        return pltpu.make_async_copy(kc_hbm.at[rows], k_ref.at[rows], s_k.at[g])

    def v_cp(g):
        rows = pl.ds(g * GROUP * SEQ, GROUP * SEQ)
        return pltpu.make_async_copy(vc_hbm.at[rows], v_ref.at[rows], s_v.at[g])

    def wo_cp(i):
        rows = pl.ds(i * 256, 256)
        return pltpu.make_async_copy(wo_hbm.at[rows], wo.at[rows], s_wo.at[i])

    def start_w(i):
        @pl.when(i < NOWN)
        def _():
            wq_cp(i).start()

        @pl.when((i == NOWN) & (c == 0))
        def _():
            pltpu.make_async_copy(wk_hbm, wbuf.at[NOWN], s_w.at[NOWN]).start()

        @pl.when((i == NOWN) & (c == 1))
        def _():
            pltpu.make_async_copy(wv_hbm, wbuf.at[NOWN], s_w.at[NOWN]).start()

        @pl.when(i > NOWN)
        def _():
            k_cp(i - NW).start()
            v_cp(i - NW).start()

    for i in range(AHEAD):
        wq_cp(i).start()
    wp_cp.start()
    vl_cp.start()

    barrier = pltpu.get_barrier_semaphore()
    for peer in (sib, xp):
        pl.semaphore_signal(barrier, inc=1, device_id={'sp': peer}, device_id_type=MESH)

    hid_cp.wait()
    pl.semaphore_wait(barrier, 2)

    def spread(slot, q):
        for h in range(2):
            qf[h, pl.ds(slot, ROWS, stride=HEADS), :] = q[:, h * 128:(h + 1) * 128]

    def slot(i, chip, core):
        h = head(i, chip)
        return 8 * (h // 4) + 4 * core + h % 4

    def q_core(i):
        return remote(qsend.at[i], qrecv.at[i], qs.at[i], qr.at[i], sib)

    def q_chip(i):
        return remote(qsend.at[i], qchip.at[i], qxs.at[i], qxr.at[i], xp)

    def q_relay(i):
        return remote(qchip.at[i], qrecv.at[NW + i], qs.at[NW + i], qr.at[NW + i], sib)

    def project(i):
        pltpu.make_async_copy(wk_hbm, wbuf.at[i], s_w.at[i]).wait()
        start_w(i + AHEAD)
        res = jnp.dot(hid[...], wbuf[i], preferred_element_type=F32).astype(BF16)
        qsend[i] = res
        q_core(i).start()
        return res.astype(F32)

    def head_step(i, _):
        res = project(i)

        @pl.when(i < SHARED)
        def _():
            q_chip(i).start()

        spread(slot(i, x, c), res)
        return 0

    lax.fori_loop(0, NOWN, head_step, 0)
    for i in range(SHARED):
        q_chip(i).wait_recv()
        q_relay(i).start()
    kvn[c] = project(NOWN)
    for g in range(AHEAD, 8):
        k_cp(g).start()
        v_cp(g).start()
    for i in range(SHARED):
        spread(slot(i, 1 - x, c), qchip[i].astype(F32))

    def take_head(i, _):
        q_core(i).wait_recv()
        spread(slot(i, x, 1 - c), qrecv[i].astype(F32))
        return 0

    lax.fori_loop(0, NOWN, take_head, 0)
    for i in range(SHARED):
        q_relay(i).wait_recv()
        spread(slot(i, 1 - x, 1 - c), qrecv[NW + i].astype(F32))
    q_core(NOWN).wait_recv()
    kvn[1 - c] = qrecv[NOWN].astype(F32)
    wp_cp.wait()
    vl_cp.wait()

    sub = lax.broadcasted_iota(jnp.int32, (8, HD), 0)
    sub1 = lax.broadcasted_iota(jnp.int32, (8, 128), 0)
    lane1 = lax.broadcasted_iota(jnp.int32, (8, 128), 1)
    lane = lax.broadcasted_iota(jnp.int32, (HEADS, SEQ), 1)

    def cache_rows(b):
        return pl.ds(pl.multiple_of(b * SEQ, SEQ), SEQ)

    def weigh(b, j):
        rows = pl.ds(pl.multiple_of(b * HEADS, HEADS), HEADS)
        q = jnp.concatenate([qf[0, rows, :], qf[1, rows, :]], axis=1)
        s = lax.dot_general(q.astype(BF16), k_ref[cache_rows(b), :], (((1,), (1,)), ((), ())),
                            preferred_element_type=F32)
        s_new = jnp.sum(q * kvn[0, pl.ds(b, 1), :], axis=1, keepdims=True)
        here = lane == wp[b] - first_pos
        s = jnp.where(here, s_new, s) * (HD ** -0.5)
        s = jnp.where(lane < vl[b] - first_pos, s, -jnp.inf)
        m = jnp.maximum(jnp.max(s, axis=1, keepdims=True), LOWEST)
        p = jnp.exp(s - m)
        l = jnp.sum(p, axis=1, keepdims=True)
        p_new = jnp.sum(jnp.where(here, p, 0.0), axis=1, keepdims=True)
        mine = slice(j * HEADS, (j + 1) * HEADS)
        prob[mine, :] = jnp.where(here, 0.0, p).astype(BF16)
        pnew[mine, :] = jnp.broadcast_to(p_new, (HEADS, 128))
        return jnp.broadcast_to(m, (HEADS, 128)), jnp.broadcast_to(l, (HEADS, 128))

    def value_sum(b, j):
        mine = slice(j * HEADS, (j + 1) * HEADS)
        o = jnp.dot(prob[mine, :], v_ref[cache_rows(b), :], preferred_element_type=F32)
        p_new = pnew[mine, :]
        return o + jnp.concatenate([p_new, p_new], axis=1) * kvn[1, pl.ds(b, 1), :]

    def pack(t0, t1, low):
        return (jnp.where(low, t0, pltpu.roll(t1, 4, 0)), jnp.where(low, pltpu.roll(t0, 4, 0), t1))

    def chunk_attention(ch, between):
        for g2 in range(CHUNK // GROUP):
            k_cp(ch * (CHUNK // GROUP) + g2).wait()

        @pl.when(ch >= 0)
        def _():
            tiles = [jnp.zeros((8, 128), F32)] * 4
            for p in range(NPAIR):
                m0, l0 = weigh(ch * CHUNK + 2 * p, 2 * p)
                m1, l1 = weigh(ch * CHUNK + 2 * p + 1, 2 * p + 1)
                for core in range(2):
                    r = slice(8 * core, 8 * core + 8)
                    ms = pack(m0[r], m1[r], sub1 < 4)
                    ls = pack(l0[r], l1[r], sub1 < 4)
                    for xd in range(2):
                        t = jnp.where(lane1 == p, ms[xd], tiles[2 * core + xd])
                        tiles[2 * core + xd] = jnp.where(lane1 == p + 64, ls[xd], t)
            for core in range(2):
                for xd in range(2):
                    ml[core, ch, xd] = tiles[2 * core + xd]

        for g2 in range(CHUNK // GROUP):
            v_cp(ch * (CHUNK // GROUP) + g2).wait()

        @pl.when(ch >= 0)
        def _():
            for p in range(NPAIR):
                o0 = value_sum(ch * CHUNK + 2 * p, 2 * p)
                o1 = value_sum(ch * CHUNK + 2 * p + 1, 2 * p + 1)
                for core in range(2):
                    r = slice(8 * core, 8 * core + 8)
                    os = pack(o0[r], o1[r], sub < 4)
                    for xd in range(2):
                        acc[core, ch, xd, p * 8:p * 8 + 8, :] = os[xd]

    def d2d(ch):
        return (remote(acc.at[1 - c, ch], racc1.at[ch], a1s.at[ch], a1r.at[ch], sib),
                remote(ml.at[1 - c, ch], rml1.at[ch], m1s.at[ch], m1r.at[ch], sib))

    def xlink(ch):
        return (remote(acc.at[c, ch, 1 - x], racc2.at[ch], a2s.at[ch], a2r.at[ch], xp),
                remote(ml.at[c, ch, 1 - x], rml2.at[ch], m2s.at[ch], m2r.at[ch], xp))

    def scales(mla, mlb):
        top = jnp.maximum(mla, mlb)
        sa, sb = jnp.exp(mla - top), jnp.exp(mlb - top)
        total = mla * pltpu.roll(sa, 64, 1) + mlb * pltpu.roll(sb, 64, 1)
        return top, sa, sb, total

    def merge_core(ch):
        for desc in d2d(ch):
            desc.wait_recv()
        for xd in range(2):
            top, sa, sb, total = scales(ml[c, ch, xd], rml1[ch, xd])
            ml[c, ch, xd] = jnp.where(lane1 < 64, top, total)
            for p in range(NPAIR):
                r = slice(p * 8, p * 8 + 8)
                acc[c, ch, xd, r, :] = (acc[c, ch, xd, r, :] * sa[:, p:p + 1]
                                        + racc1[ch, xd, r, :] * sb[:, p:p + 1])
        for desc in xlink(ch):
            desc.start()

    def merge_chip(ch):
        for desc in xlink(ch):
            desc.wait_recv()
        top, sa, sb, total = scales(ml[c, ch, x], rml2[ch])
        inv = pltpu.roll(1.0 / jnp.where(lane1 < 64, 1.0, total), 64, 1)
        sa, sb = sa * inv, sb * inv
        for p in range(NPAIR):
            r = slice(p * 8, p * 8 + 8)
            o = acc[c, ch, x, r, :] * sa[:, p:p + 1] + racc2[ch, r, :] * sb[:, p:p + 1]
            for h in range(2):
                osum[h, pl.ds(pl.multiple_of(ch * CR + p * 8, 8), 8), :] = o[:, h * 128:(h + 1) * 128]

    def core_sum(t, xd):
        return remote(pd.at[t, xd], rd.at[t, xd], rds.at[2 * t + xd], rdr.at[2 * t + xd], sib)

    def chip_sum(t):
        return remote(px.at[t], rx.at[t], rxs.at[t], rxr.at[t], xp)

    def project_block(dst, t, j):
        rows = pl.ds(pl.multiple_of(t * OUT, OUT), OUT)
        cols = pl.ds(pl.multiple_of(j * BLK, BLK), BLK)
        dst[...] = jnp.dot(obf[rows, :], wo[:, cols], preferred_element_type=F32)

    def project_far(t):
        rows = pl.ds(pl.multiple_of(t * OUT, OUT), OUT)
        for r in range(4):
            for h in range(2):
                lanes = slice(r * HD + h * 128, r * HD + (h + 1) * 128)
                obf[rows, lanes] = osum[h, pl.ds(t * 4 * OUT + r, OUT, stride=4), :].astype(BF16)
        project_block(pd.at[t, 0], t, 2 * (1 - x) + 1 - c)
        project_block(px.at[t], t, 2 * (1 - x) + c)
        core_sum(t, 0).start()

    def project_near(t):
        project_block(pd.at[t, 1], t, 2 * x + 1 - c)
        project_block(pk.at[t], t, 2 * x + c)
        core_sum(t, 1).start()

    def send_far(t):
        core_sum(t, 0).wait_recv()
        px[t] = px[t] + rd[t, 0]
        chip_sum(t).start()

    def finish(t):
        core_sum(t, 1).wait_recv()
        chip_sum(t).wait_recv()
        out_ref[pl.ds(pl.multiple_of(t * OUT, OUT), OUT), :] = ((pk[t] + rd[t, 1]) + rx[t]).astype(BF16)

    def pipeline(ch, _):
        def earlier():
            @pl.when(ch >= DIST)
            def _():
                merge_core(ch - DIST)

        @pl.when(ch < 4)
        def _():
            wo_cp(ch).start()

        chunk_attention(ch, earlier)
        for desc in d2d(ch):
            desc.start()
        earlier()
        return 0

    lax.fori_loop(0, NCH, pipeline, 0)

    for i in range(4):
        wo_cp(i).wait()

    def outputs(t, _):
        for u in range(OUT // CHUNK):
            merge_chip(t * (OUT // CHUNK) + u)
        project_far(t)

        @pl.when(t == NOUT - 1)
        def _():
            send_far(t - 1)

        project_near(t)

        @pl.when(t == 0)
        def _():
            merge_core(NCH - 1)

        @pl.when((t > 0) & (t < NOUT - 1))
        def _():
            send_far(t - 1)
        return 0

    lax.fori_loop(0, NOUT, outputs, 0)
    send_far(NOUT - 1)

    def end_q(i, _):
        q_core(i).wait_send()
        return 0

    lax.fori_loop(0, NW, end_q, 0)
    for i in range(SHARED):
        q_chip(i).wait_send()
        q_relay(i).wait_send()

    def end_chunk(ch, _):
        for desc in d2d(ch) + xlink(ch):
            desc.wait_send()
        return 0

    lax.fori_loop(0, NCH, end_chunk, 0)

    def end_out(t, _):
        core_sum(t, 0).wait_send()
        core_sum(t, 1).wait_send()
        return 0

    lax.fori_loop(0, NOUT, end_out, 0)

    def finals(t, _):
        finish(t)
        chip_sum(t).wait_send()
        return 0

    lax.fori_loop(0, NOUT, finals, 0)


def cache_kernel(wp, kvn, k_in, v_in, k_ref, v_ref, k_out, v_out, s_k, s_v):
    first_pos = lax.axis_index('sp') * SEQ
    row = lax.broadcasted_iota(jnp.int32, (16, HD), 0)

    def insert(g):
        for j in range(GROUP):
            b = g * GROUP + j
            pos = wp[b] - first_pos
            base = jnp.clip(pos, 0, SEQ - 1) // 16 * 16
            rows = pl.ds(pl.multiple_of(b * SEQ + base, 16), 16)
            hit = row == pos - base
            for ref, i in ((k_ref, 0), (v_ref, 1)):
                ref[rows, :] = jnp.where(hit, kvn[i, pl.ds(b, 1), :], ref[rows, :].astype(F32)).astype(BF16)

    def copies(g):
        rows = pl.ds(g * GROUP * SEQ, GROUP * SEQ)
        return (pltpu.make_async_copy(k_ref.at[rows], k_out.at[rows], s_k.at[g]),
                pltpu.make_async_copy(v_ref.at[rows], v_out.at[rows], s_v.at[g]))

    for g in range(9):
        if g < 8:
            insert(g)
        if g >= 1:
            for cp in copies(g - 1):
                cp.start()
    for g in range(8):
        for cp in copies(g):
            cp.wait()


def join_kernel(b0, b1, b2, b3, out, sems):
    sp = lax.axis_index('sp')
    x, c = sp // 2, sp % 2
    copies = []
    for i, ref in enumerate((b0, b1, b2, b3)):
        j = 2 * (x if i < 2 else 1 - x) + (c if i % 2 == 0 else 1 - c)
        cols = pl.ds(pl.multiple_of(j * BLK, BLK), BLK)
        copies.append(pltpu.make_async_copy(ref, out.at[:, cols], sems.at[i]))
    for cp in copies:
        cp.start()
    for cp in copies:
        cp.wait()


def solution(mesh):
    row_spec = P(('rep', 'dp'), None)
    cache_spec = P(('rep', 'dp'), 'sp', None, None)
    len_spec = P(('rep', 'dp'))

    def local_step(hidden, w_query, w_key, w_value, w_out, k_cache, v_cache, write_pos, valid_len):
        flat = (ROWS * SEQ, HD)
        args = (hidden, w_query, w_key, w_value, w_out, k_cache.reshape(flat), v_cache.reshape(flat),
                write_pos, valid_len)
        args = tuple(pltpu.with_memory_space_constraint(a, pltpu.HBM) for a in args)
        vm = pl.BlockSpec(memory_space=pltpu.VMEM)
        dma = pltpu.SemaphoreType.DMA
        out, k_old, v_old, kv_new = pl.pallas_call(
            step_kernel,
            out_shape=[pltpu.VMEM((ROWS, BLK), BF16), pltpu.VMEM(flat, BF16), pltpu.VMEM(flat, BF16),
                       pltpu.VMEM((2, ROWS, HD), F32)],
            in_specs=[pl.BlockSpec(memory_space=pltpu.HBM)] * 9,
            out_specs=[vm, vm, vm, vm],
            scratch_shapes=[
                pltpu.VMEM((ROWS, DIM), BF16),
                pltpu.VMEM((NW, DIM, HD), BF16),
                pltpu.VMEM((BLK, DIM), BF16),
                pltpu.SMEM((ROWS,), jnp.int32),
                pltpu.SMEM((ROWS,), jnp.int32),
                pltpu.VMEM((2, ROWS * HEADS, 128), F32),
                pltpu.VMEM((NW, ROWS, HD), BF16),
                pltpu.VMEM((NW + SHARED, ROWS, HD), BF16),
                pltpu.VMEM((SHARED, ROWS, HD), BF16),
                pltpu.VMEM((CHUNK * HEADS, SEQ), BF16),
                pltpu.VMEM((CHUNK * HEADS, 128), F32),
                pltpu.VMEM((2, NCH, 2, CR, HD), F32),
                pltpu.VMEM((2, NCH, 2, 8, 128), F32),
                pltpu.VMEM((NCH, 2, CR, HD), F32),
                pltpu.VMEM((NCH, 2, 8, 128), F32),
                pltpu.VMEM((NCH, CR, HD), F32),
                pltpu.VMEM((NCH, 8, 128), F32),
                pltpu.VMEM((2, 4 * ROWS, 128), F32),
                pltpu.VMEM((ROWS, BLK), BF16),
                pltpu.VMEM((NOUT, 2, OUT, BLK), F32),
                pltpu.VMEM((NOUT, OUT, BLK), F32),
                pltpu.VMEM((NOUT, OUT, BLK), F32),
                pltpu.VMEM((NOUT, 2, OUT, BLK), F32),
                pltpu.VMEM((NOUT, OUT, BLK), F32),
                dma((3,)), dma((NW,)), dma((8,)), dma((8,)), dma((4,)),
                dma((NW + SHARED,)), dma((NW + SHARED,)), dma((SHARED,)), dma((SHARED,)),
                dma((NCH,)), dma((NCH,)), dma((NCH,)), dma((NCH,)),
                dma((NCH,)), dma((NCH,)), dma((NCH,)), dma((NCH,)),
                dma((2 * NOUT,)), dma((2 * NOUT,)), dma((NOUT,)), dma((NOUT,)),
            ],
            compiler_params=pltpu.CompilerParams(
                vmem_limit_bytes=44 * 2 ** 20, collective_id=0, has_side_effects=True),
            name='decode_step',
        )(*args)
        anywhere = pl.BlockSpec(memory_space=pltpu.HBM)
        others = [lax.ppermute(out, 'sp', [(i, i ^ j) for i in range(4)]) for j in (1, 2, 3)]
        others = [pltpu.with_memory_space_constraint(o, pltpu.VMEM) for o in others]
        _, _, k_new, v_new = pl.pallas_call(
            cache_kernel,
            out_shape=[pltpu.VMEM(flat, BF16), pltpu.VMEM(flat, BF16),
                       pltpu.HBM(flat, BF16), pltpu.HBM(flat, BF16)],
            in_specs=[pl.BlockSpec(memory_space=pltpu.SMEM), vm, vm, vm],
            out_specs=[vm, vm, anywhere, anywhere],
            scratch_shapes=[dma((8,)), dma((8,))],
            input_output_aliases={2: 0, 3: 1},
            cost_estimate=pl.CostEstimate(flops=2 ** 33, bytes_accessed=2 ** 25, transcendentals=0),
            compiler_params=pltpu.CompilerParams(vmem_limit_bytes=2 ** 20),
            name='cache_update',
        )(write_pos, kv_new, k_old, v_old)
        attn_out = pl.pallas_call(
            join_kernel,
            out_shape=pltpu.HBM((ROWS, DIM), BF16),
            in_specs=[vm] * 4,
            out_specs=anywhere,
            scratch_shapes=[dma((4,))],
            compiler_params=pltpu.CompilerParams(vmem_limit_bytes=2 ** 20),
            name='join',
        )(out, *others)
        return attn_out, k_new.reshape(k_cache.shape), v_new.reshape(v_cache.shape)

    return jax.shard_map(local_step, mesh=mesh, in_specs=(row_spec, P(), P(), P(), P('sp', None), cache_spec, cache_spec, len_spec, len_spec), out_specs=(row_spec, cache_spec, cache_spec), check_vma=False)
```

```python
import jax
import jax.numpy as jnp
from jax import lax
from jax.experimental import pallas as pl
from jax.experimental.pallas import tpu as pltpu
from jax.sharding import PartitionSpec as P

MESH = pl.DeviceIdType.MESH
F32, BF16 = jnp.float32, jnp.bfloat16
LOWEST = float(jnp.finfo(jnp.float32).min)

ROWS = 64
SEQ = 256
DIM = 4096
HD = 256
HEADS = 16
GROUP = 8
CHUNK = 16
NCH = ROWS // CHUNK
NPAIR = CHUNK // 2
CR = NPAIR * 8
OUT = 16
NOUT = ROWS // OUT
BLK = 1024
SPLIT = 5
AHEAD = 4
SHARED = 3
RELAY = 2
NOWN = 8 - SHARED
NW = NOWN + 1
DIST = 1


def step_kernel(hid_hbm, wq_hbm, wk_hbm, wv_hbm, wo_hbm, kc_hbm, vc_hbm, wp_hbm, vl_hbm,
                out_ref, k_ref, v_ref, kvn, wp,
                hid, wbuf, wo, vl, qf, qsend, qrecv, qchip, prob, pnew,
                acc, racc1, racc2, rml2, osum, obf,
                pd, rd, px, rx, pn, rn, pk,
                s_in, s_w, s_k, s_v, s_wo,
                qs, qr, qxs, qxr, qrs, qrr, a1s, a1r, a2s, a2r, m2s, m2r,
                f_s, f_r, n_s, n_r, rxs, rxr):
    sp = lax.axis_index('sp')
    x, c = sp // 2, sp % 2
    sib = 2 * x + (1 - c)
    xp = 2 * (1 - x) + c
    diag = 2 * (1 - x) + 1 - c
    first_pos = sp * SEQ

    def remote(src, dst, ss, rs, peer):
        return pltpu.make_async_remote_copy(src_ref=src, dst_ref=dst, send_sem=ss, recv_sem=rs,
                                            device_id={'sp': peer}, device_id_type=MESH)

    hid_cp = pltpu.make_async_copy(hid_hbm, hid, s_in.at[0])
    wp_cp = pltpu.make_async_copy(wp_hbm, wp, s_in.at[1])
    vl_cp = pltpu.make_async_copy(vl_hbm, vl, s_in.at[2])
    hid_cp.start()

    def head(i, chip):
        return i + chip * (7 - 2 * i)

    def wq_cp(i):
        cols = pl.ds(pl.multiple_of((8 * c + head(i, x)) * HD, HD), HD)
        return pltpu.make_async_copy(wq_hbm.at[:, cols], wbuf.at[i], s_w.at[i % AHEAD])

    def k_cp(g):
        rows = pl.ds(g * CHUNK * SEQ, CHUNK * SEQ)
        return pltpu.make_async_copy(kc_hbm.at[rows], k_ref.at[rows], s_k.at[g])

    def v_cp(g):
        rows = pl.ds(g * CHUNK * SEQ, CHUNK * SEQ)
        return pltpu.make_async_copy(vc_hbm.at[rows], v_ref.at[rows], s_v.at[g])

    def wo_cp(i):
        rows = pl.ds(i * 256, 256)
        return pltpu.make_async_copy(wo_hbm.at[rows], wo.at[rows], s_wo.at[0])

    def start_w(i):
        @pl.when(i < NOWN)
        def _():
            wq_cp(i).start()

        @pl.when((i == NOWN) & (c == 0))
        def _():
            pltpu.make_async_copy(wk_hbm, wbuf.at[NOWN], s_w.at[NOWN % AHEAD]).start()

        @pl.when((i == NOWN) & (c == 1))
        def _():
            pltpu.make_async_copy(wv_hbm, wbuf.at[NOWN], s_w.at[NOWN % AHEAD]).start()

        @pl.when((i > NOWN) & (i < NW + NCH))
        def _():
            k_cp(i - NW).start()
            v_cp(i - NW).start()

    for i in range(AHEAD):
        wq_cp(i).start()
    wp_cp.start()
    vl_cp.start()

    barrier = pltpu.get_barrier_semaphore()
    for peer in (sib, xp, diag):
        pl.semaphore_signal(barrier, inc=1, device_id={'sp': peer}, device_id_type=MESH)

    hid_cp.wait()
    pl.semaphore_wait(barrier, 3)

    def spread(slot, q):
        for h in range(2):
            qf[h, pl.ds(slot, ROWS, stride=HEADS), :] = q[:, h * 128:(h + 1) * 128]

    def slot(i, chip, core):
        h = head(i, chip)
        return 8 * (h // 4) + 4 * core + h % 4

    def q_core(i):
        return remote(qsend.at[i], qrecv.at[i], qs.at[0], qr.at[0], sib)

    def q_chip(i):
        return remote(qsend.at[i], qchip.at[i], qxs.at[0], qxr.at[i], xp)

    def q_far(i):
        return remote(qsend.at[i], qrecv.at[NW + i], qxs.at[0], qrr.at[0], diag)

    def q_relay(i):
        return remote(qchip.at[i], qrecv.at[NW + i], qrs.at[0], qrr.at[0], sib)

    def project(i):
        pltpu.make_async_copy(wk_hbm, wbuf.at[i], s_w.at[i % AHEAD]).wait()
        start_w(i + AHEAD)
        res = jnp.dot(hid[...], wbuf[i], preferred_element_type=F32).astype(BF16)
        qsend[i] = res
        q_core(i).start()
        return res.astype(F32)

    def head_step(i, _):
        res = project(i)

        @pl.when(i < SHARED)
        def _():
            q_chip(i).start()

        @pl.when((i >= RELAY) & (i < SHARED))
        def _():
            q_far(i).start()

        spread(slot(i, x, c), res)
        return 0

    lax.fori_loop(0, NOWN, head_step, 0)
    for g in range(NCH + NW - AHEAD - NW, NCH):
        if g + NW >= NW + AHEAD:
            k_cp(g).start()
            v_cp(g).start()
    kvn[c] = project(NOWN)
    for i in range(RELAY):
        q_chip(i).wait_recv()
        q_relay(i).start()
    for i in range(SHARED):
        if i >= RELAY:
            q_chip(i).wait_recv()
        spread(slot(i, 1 - x, c), qchip[i].astype(F32))
    remote(qsend, qrecv.at[pl.ds(0, NW)], qs.at[0], qr.at[0], sib).wait_recv()
    kvn[1 - c] = qrecv[NOWN].astype(F32)

    def take_head(i, _):
        spread(slot(i, x, 1 - c), qrecv[i].astype(F32))
        return 0

    lax.fori_loop(0, NOWN, take_head, 0)
    remote(qchip, qrecv.at[pl.ds(NW, SHARED)], qrs.at[0], qrr.at[0], sib).wait_recv()
    for i in range(SHARED):
        spread(slot(i, 1 - x, 1 - c), qrecv[NW + i].astype(F32))
    wp_cp.wait()
    vl_cp.wait()

    sub = lax.broadcasted_iota(jnp.int32, (8, HD), 0)
    sub1 = lax.broadcasted_iota(jnp.int32, (8, 128), 0)
    lane1 = lax.broadcasted_iota(jnp.int32, (8, 128), 1)
    lane = lax.broadcasted_iota(jnp.int32, (HEADS, SEQ), 1)

    def cache_rows(b):
        return pl.ds(pl.multiple_of(b * SEQ, SEQ), SEQ)

    def weigh(b, j):
        rows = pl.ds(pl.multiple_of(b * HEADS, HEADS), HEADS)
        q = jnp.concatenate([qf[0, rows, :], qf[1, rows, :]], axis=1)
        s = lax.dot_general(q.astype(BF16), k_ref[cache_rows(b), :], (((1,), (1,)), ((), ())),
                            preferred_element_type=F32)
        s_new = jnp.sum(q * kvn[0, pl.ds(b, 1), :], axis=1, keepdims=True)
        here = lane == wp[b] - first_pos
        s = jnp.where(here, s_new, s) * (HD ** -0.5)
        s = jnp.where(lane < vl[b] - first_pos, s, -jnp.inf)
        m = jnp.maximum(jnp.max(s, axis=1, keepdims=True), LOWEST)
        p = jnp.exp(s - m)
        l = jnp.sum(p, axis=1, keepdims=True)
        p_new = jnp.sum(jnp.where(here, p, 0.0), axis=1, keepdims=True)
        mine = slice(j * HEADS, (j + 1) * HEADS)
        prob[mine, :] = jnp.where(here, 0.0, p).astype(BF16)
        pnew[mine, :] = jnp.broadcast_to(p_new, (HEADS, 128))
        return jnp.broadcast_to(m, (HEADS, 128)), jnp.broadcast_to(l, (HEADS, 128))

    def value_sum(b, j):
        mine = slice(j * HEADS, (j + 1) * HEADS)
        o = jnp.dot(prob[mine, :], v_ref[cache_rows(b), :], preferred_element_type=F32)
        p_new = pnew[mine, :]
        return o + jnp.concatenate([p_new, p_new], axis=1) * kvn[1, pl.ds(b, 1), :]

    def pack(t0, t1, low):
        return (jnp.where(low, t0, pltpu.roll(t1, 4, 0)), jnp.where(low, pltpu.roll(t0, 4, 0), t1))

    def chunk_attention(ch, between):
        k_cp(ch).wait()

        @pl.when(ch >= 0)
        def _():
            tiles = [jnp.zeros((8, 128), F32)] * 4
            for p in range(NPAIR):
                m0, l0 = weigh(ch * CHUNK + 2 * p, 2 * p)
                m1, l1 = weigh(ch * CHUNK + 2 * p + 1, 2 * p + 1)
                for core in range(2):
                    r = slice(8 * core, 8 * core + 8)
                    ms = pack(m0[r], m1[r], sub1 < 4)
                    ls = pack(l0[r], l1[r], sub1 < 4)
                    for xd in range(2):
                        t = jnp.where(lane1 == p, ms[xd], tiles[2 * core + xd])
                        tiles[2 * core + xd] = jnp.where(lane1 == p + 64, ls[xd], t)
            for core in range(2):
                acc[core, ch, 2 * CR:, :] = jnp.concatenate(tiles[2 * core:2 * core + 2], axis=1)

        v_cp(ch).wait()

        @pl.when(ch >= 0)
        def _():
            for p in range(NPAIR):
                o0 = value_sum(ch * CHUNK + 2 * p, 2 * p)
                o1 = value_sum(ch * CHUNK + 2 * p + 1, 2 * p + 1)
                for core in range(2):
                    r = slice(8 * core, 8 * core + 8)
                    os = pack(o0[r], o1[r], sub < 4)
                    for xd in range(2):
                        acc[core, ch, xd * CR + p * 8:xd * CR + p * 8 + 8, :] = os[xd]

    def d2d(ch):
        return remote(acc.at[1 - c, ch], racc1.at[ch], a1s.at[0], a1r.at[ch], sib)

    def xlink(ch):
        sums = pl.ds(pl.multiple_of((1 - x) * CR, 8), CR)
        lanes = pl.ds(pl.multiple_of((1 - x) * 128, 128), 128)
        return (remote(acc.at[c, ch, sums], racc2.at[ch], a2s.at[0], a2r.at[ch], xp),
                remote(acc.at[c, ch, pl.ds(2 * CR, 8), lanes], rml2.at[ch], m2s.at[0], m2r.at[ch], xp))

    def scales(mla, mlb):
        top = jnp.maximum(mla, mlb)
        sa, sb = jnp.exp(mla - top), jnp.exp(mlb - top)
        total = mla * pltpu.roll(sa, 64, 1) + mlb * pltpu.roll(sb, 64, 1)
        return top, sa, sb, total

    def merge_core(ch):
        d2d(ch).wait_recv()
        for xd in range(2):
            lanes = slice(xd * 128, xd * 128 + 128)
            top, sa, sb, total = scales(acc[c, ch, 2 * CR:, lanes], racc1[ch, 2 * CR:, lanes])
            acc[c, ch, 2 * CR:, lanes] = jnp.where(lane1 < 64, top, total)
            for p in range(NPAIR):
                r = slice(xd * CR + p * 8, xd * CR + p * 8 + 8)
                acc[c, ch, r, :] = acc[c, ch, r, :] * sa[:, p:p + 1] + racc1[ch, r, :] * sb[:, p:p + 1]
        for desc in xlink(ch):
            desc.start()

    def merge_chip(ch):
        for desc in xlink(ch):
            desc.wait_recv()
        lanes = pl.ds(pl.multiple_of(x * 128, 128), 128)
        top, sa, sb, total = scales(acc[c, ch, 2 * CR:, lanes], rml2[ch])
        inv = pltpu.roll(1.0 / jnp.where(lane1 < 64, 1.0, total), 64, 1)
        sa, sb = sa * inv, sb * inv
        for p in range(NPAIR):
            mine = pl.ds(pl.multiple_of(x * CR + p * 8, 8), 8)
            o = acc[c, ch, mine, :] * sa[:, p:p + 1] + racc2[ch, p * 8:p * 8 + 8, :] * sb[:, p:p + 1]
            for h in range(2):
                osum[h, pl.ds(pl.multiple_of(ch * CR + p * 8, 8), 8), :] = o[:, h * 128:(h + 1) * 128]

    def far_sum(t):
        return remote(pd.at[t], rd.at[t], f_s.at[0], f_r.at[t], sib)

    def near_sum():
        return remote(pn, rn, n_s.at[0], n_r.at[0], sib)

    def chip_sum(t):
        return remote(px.at[t], rx.at[t], rxs.at[0], rxr.at[0], xp)

    def project_block(dst, rows, j):
        cols = pl.ds(pl.multiple_of(j * BLK, BLK), BLK)
        dst[...] = jnp.dot(obf[rows, :], wo[:, cols], preferred_element_type=F32)

    def project_far(t):
        rows = pl.ds(pl.multiple_of(t * OUT, OUT), OUT)
        for r in range(4):
            for h in range(2):
                lanes = slice(r * HD + h * 128, r * HD + (h + 1) * 128)
                obf[rows, lanes] = osum[h, pl.ds(t * 4 * OUT + r, OUT, stride=4), :].astype(BF16)
        project_block(pd.at[t], rows, diag)
        project_block(px.at[t], rows, xp)
        far_sum(t).start()

    def project_near():
        project_block(pn, pl.ds(0, ROWS), sib)
        project_block(pk, pl.ds(0, ROWS), sp)
        near_sum().start()

    def send_far(t):
        far_sum(t).wait_recv()
        px[t] = px[t] + rd[t]
        chip_sum(t).start()

    def pipeline(ch, _):
        def earlier():
            @pl.when(ch >= DIST)
            def _():
                merge_core(ch - DIST)

        @pl.when(ch < 4)
        def _():
            wo_cp(ch).start()

        chunk_attention(ch, earlier)
        d2d(ch).start()
        earlier()
        return 0

    lax.fori_loop(0, NCH, pipeline, 0)

    pltpu.make_async_copy(wo_hbm, wo, s_wo.at[0]).wait()

    def outputs(t, _):
        for u in range(OUT // CHUNK):
            merge_chip(t * (OUT // CHUNK) + u)
        project_far(t)

        @pl.when(t > 0)
        def _():
            send_far(t - 1)
        return 0

    merge_core(NCH - 1)
    lax.fori_loop(0, NOUT, outputs, 0)
    project_near()
    send_far(NOUT - 1)

    remote(qsend, qrecv.at[pl.ds(0, NW)], qs.at[0], qr.at[0], sib).wait_send()
    n_far = 2 * SHARED - RELAY
    remote(qrecv.at[pl.ds(0, n_far)], qrecv.at[pl.ds(0, n_far)], qxs.at[0], qxr.at[0], xp).wait_send()
    remote(qchip.at[pl.ds(0, RELAY)], qrecv.at[pl.ds(0, RELAY)], qrs.at[0], qrr.at[0], sib).wait_send()
    remote(acc.at[1 - c], racc1, a1s.at[0], a1r.at[0], sib).wait_send()
    remote(racc2, racc2, a2s.at[0], a2r.at[0], xp).wait_send()
    remote(rml2, rml2, m2s.at[0], m2r.at[0], xp).wait_send()
    remote(px, rx, f_s.at[0], f_r.at[0], sib).wait_send()
    near_sum().wait_send()

    near_sum().wait_recv()
    remote(px, rx, rxs.at[0], rxr.at[0], xp).wait_recv()
    for t in range(NOUT):
        r = slice(t * OUT, (t + 1) * OUT)
        out_ref[r, :] = ((pk[r, :] + rn[r, :]) + rx[t]).astype(BF16)
    remote(px, rx, rxs.at[0], rxr.at[0], xp).wait_send()


def insert_rows(wp, kvn, first_pos, ref, i, groups):
    row = lax.broadcasted_iota(jnp.int32, (16, HD), 0)
    for b in range(groups.start * GROUP, groups.stop * GROUP):
        pos = wp[b] - first_pos
        base = jnp.clip(pos, 0, SEQ - 1) // 16 * 16
        rows = pl.ds(pl.multiple_of(b * SEQ + base, 16), 16)
        ref[rows, :] = jnp.where(row == pos - base, kvn[i, pl.ds(b, 1), :], ref[rows, :].astype(F32)).astype(BF16)


def copy_group(ref, out, sem, g):
    rows = pl.ds(g * GROUP * SEQ, GROUP * SEQ)
    return pltpu.make_async_copy(ref.at[rows], out.at[rows], sem)


def cache_kernel(wp, kvn, k_in, v_in, k_ref, v_ref, k_out, v_out, sems):
    first_pos = lax.axis_index('sp') * SEQ
    copies = []
    for g in range(9):
        if g < 8:
            insert_rows(wp, kvn, first_pos, k_ref, 0, range(g, g + 1))
            insert_rows(wp, kvn, first_pos, v_ref, 1, range(g, g + 1))
        if g >= 1:
            copies.append(copy_group(k_ref, k_out, sems.at[len(copies)], g - 1))
            copies[-1].start()
            if g <= SPLIT:
                copies.append(copy_group(v_ref, v_out, sems.at[len(copies)], g - 1))
                copies[-1].start()
    for cp in copies:
        cp.wait()


def rest_kernel(v_ref, token, v_in, v_out, sems):
    copies = [copy_group(v_ref, v_out, sems.at[g], g) for g in range(SPLIT, 8)]
    for cp in copies:
        cp.start()
    for cp in copies:
        cp.wait()


def join_kernel(b0, b1, b2, b3, out, sems):
    sp = lax.axis_index('sp')
    x, c = sp // 2, sp % 2
    copies = []
    for i, ref in enumerate((b0, b1, b2, b3)):
        j = 2 * (x if i < 2 else 1 - x) + (c if i % 2 == 0 else 1 - c)
        cols = pl.ds(pl.multiple_of(j * BLK, BLK), BLK)
        copies.append(pltpu.make_async_copy(ref, out.at[:, cols], sems.at[i]))
    for cp in copies:
        cp.start()
    for cp in copies:
        cp.wait()


def solution(mesh):
    row_spec = P(('rep', 'dp'), None)
    cache_spec = P(('rep', 'dp'), 'sp', None, None)
    len_spec = P(('rep', 'dp'))

    def local_step(hidden, w_query, w_key, w_value, w_out, k_cache, v_cache, write_pos, valid_len):
        flat = (ROWS * SEQ, HD)
        args = (hidden, w_query, w_key, w_value, w_out, k_cache.reshape(flat), v_cache.reshape(flat),
                write_pos, valid_len)
        args = tuple(pltpu.with_memory_space_constraint(a, pltpu.HBM) for a in args)
        vm = pl.BlockSpec(memory_space=pltpu.VMEM)
        dma = pltpu.SemaphoreType.DMA
        out, k_old, v_old, kv_new, where_to = pl.pallas_call(
            step_kernel,
            out_shape=[pltpu.VMEM((ROWS, BLK), BF16), pltpu.VMEM(flat, BF16), pltpu.VMEM(flat, BF16),
                       pltpu.VMEM((2, ROWS, HD), F32), pltpu.SMEM((ROWS,), jnp.int32)],
            in_specs=[pl.BlockSpec(memory_space=pltpu.HBM)] * 9,
            out_specs=[vm, vm, vm, vm, pl.BlockSpec(memory_space=pltpu.SMEM)],
            scratch_shapes=[
                pltpu.VMEM((ROWS, DIM), BF16),
                pltpu.VMEM((NW, DIM, HD), BF16),
                pltpu.VMEM((BLK, DIM), BF16),
                pltpu.SMEM((ROWS,), jnp.int32),
                pltpu.VMEM((2, ROWS * HEADS, 128), F32),
                pltpu.VMEM((NW, ROWS, HD), BF16),
                pltpu.VMEM((NW + SHARED, ROWS, HD), BF16),
                pltpu.VMEM((SHARED, ROWS, HD), BF16),
                pltpu.VMEM((CHUNK * HEADS, SEQ), BF16),
                pltpu.VMEM((CHUNK * HEADS, 128), F32),
                pltpu.VMEM((2, NCH, 2 * CR + 8, HD), F32),
                pltpu.VMEM((NCH, 2 * CR + 8, HD), F32),
                pltpu.VMEM((NCH, CR, HD), F32),
                pltpu.VMEM((NCH, 8, 128), F32),
                pltpu.VMEM((2, 4 * ROWS, 128), F32),
                pltpu.VMEM((ROWS, BLK), BF16),
                pltpu.VMEM((NOUT, OUT, BLK), F32),
                pltpu.VMEM((NOUT, OUT, BLK), F32),
                pltpu.VMEM((NOUT, OUT, BLK), F32),
                pltpu.VMEM((NOUT, OUT, BLK), F32),
                pltpu.VMEM((ROWS, BLK), F32),
                pltpu.VMEM((ROWS, BLK), F32),
                pltpu.VMEM((ROWS, BLK), F32),
                dma((3,)), dma((AHEAD,)), dma((NCH,)), dma((NCH,)), dma((1,)),
                dma((1,)), dma((1,)), dma((1,)), dma((SHARED,)), dma((1,)), dma((1,)),
                dma((1,)), dma((NCH,)), dma((1,)), dma((NCH,)), dma((1,)), dma((NCH,)),
                dma((1,)), dma((NOUT,)), dma((1,)), dma((1,)), dma((1,)), dma((1,)),
            ],
            compiler_params=pltpu.CompilerParams(
                vmem_limit_bytes=44 * 2 ** 20, collective_id=0, has_side_effects=True),
            name='decode_step',
        )(*args)
        anywhere = pl.BlockSpec(memory_space=pltpu.HBM)
        near = [(i, i ^ 1) for i in range(4)]
        chip = lax.ppermute(out, 'sp', [(i, i ^ 2) for i in range(4)])
        core = lax.ppermute(out, 'sp', near)
        far = lax.ppermute(chip, 'sp', near)
        k_full, v_full, k_new, v_new = pl.pallas_call(
            cache_kernel,
            out_shape=[pltpu.VMEM(flat, BF16), pltpu.VMEM(flat, BF16),
                       pltpu.HBM(flat, BF16), pltpu.HBM(flat, BF16)],
            in_specs=[pl.BlockSpec(memory_space=pltpu.SMEM), vm, vm, vm],
            out_specs=[vm, vm, anywhere, anywhere],
            scratch_shapes=[dma((16,))],
            input_output_aliases={2: 0, 3: 1},
            cost_estimate=pl.CostEstimate(flops=2 ** 33, bytes_accessed=2 ** 25, transcendentals=0),
            compiler_params=pltpu.CompilerParams(vmem_limit_bytes=2 ** 20),
            name='cache_update',
        )(where_to, kv_new, k_old, v_old)
        v_new = pl.pallas_call(
            rest_kernel,
            out_shape=pltpu.HBM(flat, BF16),
            in_specs=[vm, pl.BlockSpec(memory_space=pl.ANY), anywhere],
            out_specs=anywhere,
            scratch_shapes=[dma((8,))],
            input_output_aliases={2: 0},
            cost_estimate=pl.CostEstimate(flops=2 ** 33, bytes_accessed=2 ** 24, transcendentals=0),
            compiler_params=pltpu.CompilerParams(vmem_limit_bytes=2 ** 20),
            name='cache_rest',
        )(v_full, chip, v_new)
        others = [pltpu.with_memory_space_constraint(o, pltpu.VMEM) for o in (core, chip, far)]
        attn_out = pl.pallas_call(
            join_kernel,
            out_shape=pltpu.HBM((ROWS, DIM), BF16),
            in_specs=[vm] * 4,
            out_specs=anywhere,
            scratch_shapes=[dma((4,))],
            compiler_params=pltpu.CompilerParams(vmem_limit_bytes=2 ** 20),
            name='join',
        )(out, *others)
        return attn_out, k_new.reshape(k_cache.shape), v_new.reshape(v_cache.shape)

    return jax.shard_map(local_step, mesh=mesh, in_specs=(row_spec, P(), P(), P(), P('sp', None), cache_spec, cache_spec, len_spec, len_spec), out_specs=(row_spec, cache_spec, cache_spec), check_vma=False)
```

```python
import jax
import jax.numpy as jnp
from jax import lax
from jax.experimental import pallas as pl
from jax.experimental.pallas import tpu as pltpu
from jax.sharding import PartitionSpec as P

MESH = pl.DeviceIdType.MESH
F32, BF16 = jnp.float32, jnp.bfloat16
LOWEST = float(jnp.finfo(jnp.float32).min)

ROWS = 64
SEQ = 256
DIM = 4096
HD = 256
HEADS = 16
GROUP = 8
CHUNK = 16
NCH = ROWS // CHUNK
NPAIR = CHUNK // 2
CR = NPAIR * 8
OUT = 16
NOUT = ROWS // OUT
BLK = 1024
SPLIT = 6
AHEAD = 4
SHARED = 3
NOWN = 8 - SHARED
NW = NOWN + 1
DIST = 1


def step_kernel(hid_hbm, wq_hbm, wk_hbm, wv_hbm, wo_hbm, kc_hbm, vc_hbm, wp_hbm, vl_hbm,
                out_ref, k_ref, v_ref, kvn, wp,
                hid, wbuf, wo, vl, qf, qsend, qrecv, qchip, prob, pnew,
                acc, racc1, racc2, rml2, osum, obf,
                pd, rd, px, rx, pn, rn, pk,
                s_in, s_w, s_k, s_v, s_wo,
                qs, qr, qxs, qxr, qrs, qrr, a1s, a1r, a2s, a2r, m2s, m2r,
                f_s, f_r, n_s, n_r, rxs, rxr):
    sp = lax.axis_index('sp')
    x, c = sp // 2, sp % 2
    sib = 2 * x + (1 - c)
    xp = 2 * (1 - x) + 1 - c
    diag = 2 * (1 - x) + c
    part = (x + c) % 2
    first_pos = sp * SEQ

    def remote(src, dst, ss, rs, peer):
        return pltpu.make_async_remote_copy(src_ref=src, dst_ref=dst, send_sem=ss, recv_sem=rs,
                                            device_id={'sp': peer}, device_id_type=MESH)

    hid_cp = pltpu.make_async_copy(hid_hbm, hid, s_in.at[0])
    wp_cp = pltpu.make_async_copy(wp_hbm, wp, s_in.at[1])
    vl_cp = pltpu.make_async_copy(vl_hbm, vl, s_in.at[2])
    hid_cp.start()

    def head(i, chip):
        return i + chip * (7 - 2 * i)

    def wq_cp(i):
        cols = pl.ds(pl.multiple_of((8 * c + head(i, x)) * HD, HD), HD)
        return pltpu.make_async_copy(wq_hbm.at[:, cols], wbuf.at[i], s_w.at[i % AHEAD])

    def k_cp(g):
        rows = pl.ds(g * CHUNK * SEQ, CHUNK * SEQ)
        return pltpu.make_async_copy(kc_hbm.at[rows], k_ref.at[rows], s_k.at[g])

    def v_cp(g):
        rows = pl.ds(g * CHUNK * SEQ, CHUNK * SEQ)
        return pltpu.make_async_copy(vc_hbm.at[rows], v_ref.at[rows], s_v.at[g])

    def wo_cp(i):
        rows = pl.ds(i * 256, 256)
        return pltpu.make_async_copy(wo_hbm.at[rows], wo.at[rows], s_wo.at[0])

    def start_w(i):
        @pl.when(i < NOWN)
        def _():
            wq_cp(i).start()

        @pl.when((i == NOWN) & (c == 0))
        def _():
            pltpu.make_async_copy(wk_hbm, wbuf.at[NOWN], s_w.at[NOWN % AHEAD]).start()

        @pl.when((i == NOWN) & (c == 1))
        def _():
            pltpu.make_async_copy(wv_hbm, wbuf.at[NOWN], s_w.at[NOWN % AHEAD]).start()

        @pl.when((i > NOWN) & (i < NW + NCH))
        def _():
            k_cp(i - NW).start()
            v_cp(i - NW).start()

    for i in range(AHEAD):
        wq_cp(i).start()
    wp_cp.start()
    vl_cp.start()

    barrier = pltpu.get_barrier_semaphore()
    for peer in (sib, xp):
        pl.semaphore_signal(barrier, inc=1, device_id={'sp': peer}, device_id_type=MESH)

    hid_cp.wait()
    pl.semaphore_wait(barrier, 2)

    def spread(slot, q):
        for h in range(2):
            qf[h, pl.ds(slot, ROWS, stride=HEADS), :] = q[:, h * 128:(h + 1) * 128]

    def slot(i, chip, core):
        h = head(i, chip)
        return 8 * ((core + h // 4) % 2) + 4 * core + h % 4

    def q_core(i, kind):
        return remote(qsend.at[i], qrecv.at[i], qs.at[0], qr.at[kind], sib)

    def q_chip(i):
        return remote(qsend.at[i], qchip.at[i], qxs.at[0], qxr.at[i], xp)

    def q_relay(i):
        return remote(qchip.at[i], qrecv.at[NW + i], qrs.at[0], qrr.at[0], sib)

    def project(i, kind):
        pltpu.make_async_copy(wk_hbm, wbuf.at[i], s_w.at[i % AHEAD]).wait()
        start_w(i + AHEAD)
        res = jnp.dot(hid[...], wbuf[i], preferred_element_type=F32).astype(BF16)
        qsend[i] = res
        q_core(i, kind).start()
        return res.astype(F32)

    def head_step(i, _):
        res = project(i, 0)

        @pl.when(i < SHARED)
        def _():
            q_chip(i).start()

        spread(slot(i, x, c), res)
        return 0

    lax.fori_loop(0, NOWN, head_step, 0)
    kvn[c] = project(NOWN, 1)
    for i in range(SHARED):
        q_chip(i).wait_recv()
        q_relay(i).start()
    for i in range(SHARED):
        spread(slot(i, 1 - x, 1 - c), qchip[i].astype(F32))
    heads = pl.ds(0, NOWN)
    remote(qsend.at[heads], qrecv.at[heads], qs.at[0], qr.at[0], sib).wait_recv()

    def take_head(i, _):
        spread(slot(i, x, 1 - c), qrecv[i].astype(F32))
        return 0

    lax.fori_loop(0, NOWN, take_head, 0)
    remote(qchip, qrecv.at[pl.ds(NW, SHARED)], qrs.at[0], qrr.at[0], sib).wait_recv()
    for i in range(SHARED):
        spread(slot(i, 1 - x, c), qrecv[NW + i].astype(F32))
    q_core(NOWN, 1).wait_recv()
    kvn[1 - c] = qrecv[NOWN].astype(F32)
    wp_cp.wait()
    vl_cp.wait()

    sub = lax.broadcasted_iota(jnp.int32, (8, HD), 0)
    sub1 = lax.broadcasted_iota(jnp.int32, (8, 128), 0)
    lane1 = lax.broadcasted_iota(jnp.int32, (8, 128), 1)
    lane = lax.broadcasted_iota(jnp.int32, (HEADS, SEQ), 1)

    def cache_rows(b):
        return pl.ds(pl.multiple_of(b * SEQ, SEQ), SEQ)

    def weigh(b, j):
        rows = pl.ds(pl.multiple_of(b * HEADS, HEADS), HEADS)
        q = jnp.concatenate([qf[0, rows, :], qf[1, rows, :]], axis=1)
        s = lax.dot_general(q.astype(BF16), k_ref[cache_rows(b), :], (((1,), (1,)), ((), ())),
                            preferred_element_type=F32)
        s_new = jnp.sum(q * kvn[0, pl.ds(b, 1), :], axis=1, keepdims=True)
        here = lane == wp[b] - first_pos
        s = jnp.where(here, s_new, s) * (HD ** -0.5)
        s = jnp.where(lane < vl[b] - first_pos, s, -jnp.inf)
        m = jnp.maximum(jnp.max(s, axis=1, keepdims=True), LOWEST)
        p = jnp.exp(s - m)
        l = jnp.sum(p, axis=1, keepdims=True)
        p_new = jnp.sum(jnp.where(here, p, 0.0), axis=1, keepdims=True)
        mine = slice(j * HEADS, (j + 1) * HEADS)
        prob[mine, :] = jnp.where(here, 0.0, p).astype(BF16)
        pnew[mine, :] = jnp.broadcast_to(p_new, (HEADS, 128))
        return jnp.broadcast_to(m, (HEADS, 128)), jnp.broadcast_to(l, (HEADS, 128))

    def value_sum(b, j):
        mine = slice(j * HEADS, (j + 1) * HEADS)
        o = jnp.dot(prob[mine, :], v_ref[cache_rows(b), :], preferred_element_type=F32)
        p_new = pnew[mine, :]
        return o + jnp.concatenate([p_new, p_new], axis=1) * kvn[1, pl.ds(b, 1), :]

    def pack(t0, t1, low):
        return (jnp.where(low, t0, pltpu.roll(t1, 4, 0)), jnp.where(low, pltpu.roll(t0, 4, 0), t1))

    def chunk_attention(ch, between):
        k_cp(ch).wait()

        @pl.when(ch >= 0)
        def _():
            tiles = [jnp.zeros((8, 128), F32)] * 4
            for p in range(NPAIR):
                m0, l0 = weigh(ch * CHUNK + 2 * p, 2 * p)
                m1, l1 = weigh(ch * CHUNK + 2 * p + 1, 2 * p + 1)
                for core in range(2):
                    r = slice(8 * core, 8 * core + 8)
                    ms = pack(m0[r], m1[r], sub1 < 4)
                    ls = pack(l0[r], l1[r], sub1 < 4)
                    for xd in range(2):
                        t = jnp.where(lane1 == p, ms[xd], tiles[2 * core + xd])
                        tiles[2 * core + xd] = jnp.where(lane1 == p + 64, ls[xd], t)
            for core in range(2):
                acc[core, ch, 2 * CR:, :] = jnp.concatenate(tiles[2 * core:2 * core + 2], axis=1)

        v_cp(ch).wait()

        @pl.when(ch >= 0)
        def _():
            for p in range(NPAIR):
                o0 = value_sum(ch * CHUNK + 2 * p, 2 * p)
                o1 = value_sum(ch * CHUNK + 2 * p + 1, 2 * p + 1)
                for core in range(2):
                    r = slice(8 * core, 8 * core + 8)
                    os = pack(o0[r], o1[r], sub < 4)
                    for xd in range(2):
                        acc[core, ch, xd * CR + p * 8:xd * CR + p * 8 + 8, :] = os[xd]

    def d2d(ch):
        return remote(acc.at[1 - part, ch], racc1.at[ch], a1s.at[0], a1r.at[ch], sib)

    def xlink(ch):
        sums = pl.ds(pl.multiple_of((1 - x) * CR, 8), CR)
        lanes = pl.ds(pl.multiple_of((1 - x) * 128, 128), 128)
        return (remote(acc.at[part, ch, sums], racc2.at[ch], a2s.at[0], a2r.at[ch], xp),
                remote(acc.at[part, ch, pl.ds(2 * CR, 8), lanes], rml2.at[ch], m2s.at[0], m2r.at[ch], xp))

    def scales(mla, mlb):
        top = jnp.maximum(mla, mlb)
        sa, sb = jnp.exp(mla - top), jnp.exp(mlb - top)
        total = mla * pltpu.roll(sa, 64, 1) + mlb * pltpu.roll(sb, 64, 1)
        return top, sa, sb, total

    def merge_core(ch):
        d2d(ch).wait_recv()
        for xd in range(2):
            lanes = slice(xd * 128, xd * 128 + 128)
            top, sa, sb, total = scales(acc[part, ch, 2 * CR:, lanes], racc1[ch, 2 * CR:, lanes])
            acc[part, ch, 2 * CR:, lanes] = jnp.where(lane1 < 64, top, total)
            for p in range(NPAIR):
                r = slice(xd * CR + p * 8, xd * CR + p * 8 + 8)
                acc[part, ch, r, :] = acc[part, ch, r, :] * sa[:, p:p + 1] + racc1[ch, r, :] * sb[:, p:p + 1]
        for desc in xlink(ch):
            desc.start()

    def merge_chip(ch):
        for desc in xlink(ch):
            desc.wait_recv()
        lanes = pl.ds(pl.multiple_of(x * 128, 128), 128)
        top, sa, sb, total = scales(acc[part, ch, 2 * CR:, lanes], rml2[ch])
        inv = pltpu.roll(1.0 / jnp.where(lane1 < 64, 1.0, total), 64, 1)
        sa, sb = sa * inv, sb * inv
        for p in range(NPAIR):
            mine = pl.ds(pl.multiple_of(x * CR + p * 8, 8), 8)
            o = acc[part, ch, mine, :] * sa[:, p:p + 1] + racc2[ch, p * 8:p * 8 + 8, :] * sb[:, p:p + 1]
            for h in range(2):
                osum[h, pl.ds(pl.multiple_of(ch * CR + p * 8, 8), 8), :] = o[:, h * 128:(h + 1) * 128]

    def far_sum(t):
        return remote(pd.at[t], rd.at[t], f_s.at[0], f_r.at[t], sib)

    def near_sum():
        return remote(pn, rn, n_s.at[0], n_r.at[0], sib)

    def chip_sum(t):
        return remote(px.at[t], rx.at[t], rxs.at[0], rxr.at[0], xp)

    def project_block(dst, rows, j):
        cols = pl.ds(pl.multiple_of(j * BLK, BLK), BLK)
        dst[...] = jnp.dot(obf[rows, :], wo[:, cols], preferred_element_type=F32)

    def project_far(t):
        rows = pl.ds(pl.multiple_of(t * OUT, OUT), OUT)
        for r in range(4):
            for h in range(2):
                lanes = slice(r * HD + h * 128, r * HD + (h + 1) * 128)
                obf[rows, lanes] = osum[h, pl.ds(t * 4 * OUT + r, OUT, stride=4), :].astype(BF16)
        project_block(pd.at[t], rows, diag)
        project_block(px.at[t], rows, xp)
        far_sum(t).start()

    def project_near():
        project_block(pn, pl.ds(0, ROWS), sib)
        project_block(pk, pl.ds(0, ROWS), sp)
        near_sum().start()

    def send_far(t):
        far_sum(t).wait_recv()
        px[t] = px[t] + rd[t]
        chip_sum(t).start()

    def pipeline(ch, _):
        def earlier():
            @pl.when(ch >= DIST)
            def _():
                merge_core(ch - DIST)

        @pl.when(ch < 4)
        def _():
            wo_cp(ch).start()

        chunk_attention(ch, earlier)
        d2d(ch).start()
        earlier()
        return 0

    lax.fori_loop(0, NCH, pipeline, 0)

    pltpu.make_async_copy(wo_hbm, wo, s_wo.at[0]).wait()

    def outputs(t, _):
        for u in range(OUT // CHUNK):
            merge_chip(t * (OUT // CHUNK) + u)
        project_far(t)

        @pl.when(t > 0)
        def _():
            send_far(t - 1)
        return 0

    merge_core(NCH - 1)
    lax.fori_loop(0, NOUT, outputs, 0)
    project_near()
    send_far(NOUT - 1)

    remote(qsend, qrecv.at[pl.ds(0, NW)], qs.at[0], qr.at[0], sib).wait_send()
    remote(qchip, qchip, qxs.at[0], qxr.at[0], xp).wait_send()
    remote(qchip, qrecv.at[pl.ds(NW, SHARED)], qrs.at[0], qrr.at[0], sib).wait_send()
    remote(acc.at[1 - part], racc1, a1s.at[0], a1r.at[0], sib).wait_send()
    remote(racc2, racc2, a2s.at[0], a2r.at[0], xp).wait_send()
    remote(rml2, rml2, m2s.at[0], m2r.at[0], xp).wait_send()
    remote(px, rx, f_s.at[0], f_r.at[0], sib).wait_send()
    near_sum().wait_send()

    near_sum().wait_recv()
    remote(px, rx, rxs.at[0], rxr.at[0], xp).wait_recv()
    for t in range(NOUT):
        r = slice(t * OUT, (t + 1) * OUT)
        out_ref[r, :] = ((pk[r, :] + rn[r, :]) + rx[t]).astype(BF16)
    remote(px, rx, rxs.at[0], rxr.at[0], xp).wait_send()


def insert_rows(wp, kvn, first_pos, ref, i, groups):
    row = lax.broadcasted_iota(jnp.int32, (16, HD), 0)
    for b in range(groups.start * GROUP, groups.stop * GROUP):
        pos = wp[b] - first_pos
        base = jnp.clip(pos, 0, SEQ - 1) // 16 * 16
        rows = pl.ds(pl.multiple_of(b * SEQ + base, 16), 16)
        ref[rows, :] = jnp.where(row == pos - base, kvn[i, pl.ds(b, 1), :], ref[rows, :].astype(F32)).astype(BF16)


def copy_group(ref, out, sem, g):
    rows = pl.ds(g * GROUP * SEQ, GROUP * SEQ)
    return pltpu.make_async_copy(ref.at[rows], out.at[rows], sem)


def cache_kernel(wp, kvn, k_in, v_in, k_ref, v_ref, k_out, v_out, sems):
    first_pos = lax.axis_index('sp') * SEQ
    copies = []
    for g in range(9):
        if g < 8:
            insert_rows(wp, kvn, first_pos, k_ref, 0, range(g, g + 1))
            insert_rows(wp, kvn, first_pos, v_ref, 1, range(g, g + 1))
        if g >= 1:
            copies.append(copy_group(k_ref, k_out, sems.at[len(copies)], g - 1))
            copies[-1].start()
            if g <= SPLIT:
                copies.append(copy_group(v_ref, v_out, sems.at[len(copies)], g - 1))
                copies[-1].start()
    for cp in copies:
        cp.wait()


def rest_kernel(v_ref, token, v_in, v_out, sems):
    copies = [copy_group(v_ref, v_out, sems.at[g], g) for g in range(SPLIT, 8)]
    for cp in copies:
        cp.start()
    for cp in copies:
        cp.wait()


def join_kernel(b0, b1, b2, b3, out, sems):
    sp = lax.axis_index('sp')
    x, c = sp // 2, sp % 2
    copies = []
    for i, ref in enumerate((b0, b1, b2, b3)):
        j = (sp, 2 * x + 1 - c, 3 - sp, 2 * (1 - x) + c)[i]
        cols = pl.ds(pl.multiple_of(j * BLK, BLK), BLK)
        copies.append(pltpu.make_async_copy(ref, out.at[:, cols], sems.at[i]))
    for cp in copies:
        cp.start()
    for cp in copies:
        cp.wait()


def solution(mesh):
    row_spec = P(('rep', 'dp'), None)
    cache_spec = P(('rep', 'dp'), 'sp', None, None)
    len_spec = P(('rep', 'dp'))

    def local_step(hidden, w_query, w_key, w_value, w_out, k_cache, v_cache, write_pos, valid_len):
        flat = (ROWS * SEQ, HD)
        args = (hidden, w_query, w_key, w_value, w_out, k_cache.reshape(flat), v_cache.reshape(flat),
                write_pos, valid_len)
        args = tuple(pltpu.with_memory_space_constraint(a, pltpu.HBM) for a in args)
        vm = pl.BlockSpec(memory_space=pltpu.VMEM)
        dma = pltpu.SemaphoreType.DMA
        out, k_old, v_old, kv_new, where_to = pl.pallas_call(
            step_kernel,
            out_shape=[pltpu.VMEM((ROWS, BLK), BF16), pltpu.VMEM(flat, BF16), pltpu.VMEM(flat, BF16),
                       pltpu.VMEM((2, ROWS, HD), F32), pltpu.SMEM((ROWS,), jnp.int32)],
            in_specs=[pl.BlockSpec(memory_space=pltpu.HBM)] * 9,
            out_specs=[vm, vm, vm, vm, pl.BlockSpec(memory_space=pltpu.SMEM)],
            scratch_shapes=[
                pltpu.VMEM((ROWS, DIM), BF16),
                pltpu.VMEM((NW, DIM, HD), BF16),
                pltpu.VMEM((BLK, DIM), BF16),
                pltpu.SMEM((ROWS,), jnp.int32),
                pltpu.VMEM((2, ROWS * HEADS, 128), F32),
                pltpu.VMEM((NW, ROWS, HD), BF16),
                pltpu.VMEM((NW + SHARED, ROWS, HD), BF16),
                pltpu.VMEM((SHARED, ROWS, HD), BF16),
                pltpu.VMEM((CHUNK * HEADS, SEQ), BF16),
                pltpu.VMEM((CHUNK * HEADS, 128), F32),
                pltpu.VMEM((2, NCH, 2 * CR + 8, HD), F32),
                pltpu.VMEM((NCH, 2 * CR + 8, HD), F32),
                pltpu.VMEM((NCH, CR, HD), F32),
                pltpu.VMEM((NCH, 8, 128), F32),
                pltpu.VMEM((2, 4 * ROWS, 128), F32),
                pltpu.VMEM((ROWS, BLK), BF16),
                pltpu.VMEM((NOUT, OUT, BLK), F32),
                pltpu.VMEM((NOUT, OUT, BLK), F32),
                pltpu.VMEM((NOUT, OUT, BLK), F32),
                pltpu.VMEM((NOUT, OUT, BLK), F32),
                pltpu.VMEM((ROWS, BLK), F32),
                pltpu.VMEM((ROWS, BLK), F32),
                pltpu.VMEM((ROWS, BLK), F32),
                dma((3,)), dma((AHEAD,)), dma((NCH,)), dma((NCH,)), dma((1,)),
                dma((1,)), dma((2,)), dma((1,)), dma((SHARED,)), dma((1,)), dma((1,)),
                dma((1,)), dma((NCH,)), dma((1,)), dma((NCH,)), dma((1,)), dma((NCH,)),
                dma((1,)), dma((NOUT,)), dma((1,)), dma((1,)), dma((1,)), dma((1,)),
            ],
            compiler_params=pltpu.CompilerParams(
                vmem_limit_bytes=44 * 2 ** 20, collective_id=0, has_side_effects=True),
            name='decode_step',
        )(*args)
        anywhere = pl.BlockSpec(memory_space=pltpu.HBM)
        near = [(i, i ^ 1) for i in range(4)]
        chip = lax.ppermute(out, 'sp', [(i, 3 - i) for i in range(4)])
        core = lax.ppermute(out, 'sp', near)
        far = lax.ppermute(chip, 'sp', near)
        k_full, v_full, k_new, v_new = pl.pallas_call(
            cache_kernel,
            out_shape=[pltpu.VMEM(flat, BF16), pltpu.VMEM(flat, BF16),
                       pltpu.HBM(flat, BF16), pltpu.HBM(flat, BF16)],
            in_specs=[pl.BlockSpec(memory_space=pltpu.SMEM), vm, vm, vm],
            out_specs=[vm, vm, anywhere, anywhere],
            scratch_shapes=[dma((16,))],
            input_output_aliases={2: 0, 3: 1},
            cost_estimate=pl.CostEstimate(flops=2 ** 33, bytes_accessed=2 ** 25, transcendentals=0),
            compiler_params=pltpu.CompilerParams(vmem_limit_bytes=2 ** 20),
            name='cache_update',
        )(where_to, kv_new, k_old, v_old)
        v_new = pl.pallas_call(
            rest_kernel,
            out_shape=pltpu.HBM(flat, BF16),
            in_specs=[vm, pl.BlockSpec(memory_space=pl.ANY), anywhere],
            out_specs=anywhere,
            scratch_shapes=[dma((8,))],
            input_output_aliases={2: 0},
            cost_estimate=pl.CostEstimate(flops=2 ** 33, bytes_accessed=2 ** 24, transcendentals=0),
            compiler_params=pltpu.CompilerParams(vmem_limit_bytes=2 ** 20),
            name='cache_rest',
        )(v_full, chip, v_new)
        others = [pltpu.with_memory_space_constraint(o, pltpu.VMEM) for o in (core, chip, far)]
        attn_out = pl.pallas_call(
            join_kernel,
            out_shape=pltpu.HBM((ROWS, DIM), BF16),
            in_specs=[vm] * 4,
            out_specs=anywhere,
            scratch_shapes=[dma((4,))],
            compiler_params=pltpu.CompilerParams(vmem_limit_bytes=2 ** 20),
            name='join',
        )(out, *others)
        return attn_out, k_new.reshape(k_cache.shape), v_new.reshape(v_cache.shape)

    return jax.shard_map(local_step, mesh=mesh, in_specs=(row_spec, P(), P(), P(), P('sp', None), cache_spec, cache_spec, len_spec, len_spec), out_specs=(row_spec, cache_spec, cache_spec), check_vma=False)
```

```python
import jax
import jax.numpy as jnp
from jax import lax
from jax.experimental import pallas as pl
from jax.experimental.pallas import tpu as pltpu
from jax.sharding import PartitionSpec as P

MESH = pl.DeviceIdType.MESH
F32, BF16 = jnp.float32, jnp.bfloat16
LOWEST = float(jnp.finfo(jnp.float32).min)

ROWS = 64
SEQ = 256
DIM = 4096
HD = 256
HEADS = 16
GROUP = 8
CHUNK = 16
NCH = ROWS // CHUNK
NPAIR = CHUNK // 2
CR = NPAIR * 8
OUT = 16
NOUT = ROWS // OUT
BLK = 1024
SPLIT = 6
AHEAD = 4
SHARED = 3
NOWN = 8 - SHARED
NW = NOWN + 1
DIST = 1


def step_kernel(hid_hbm, wq_hbm, wk_hbm, wv_hbm, wo_hbm, kc_hbm, vc_hbm, wp_hbm, vl_hbm,
                out_ref, k_ref, v_ref, kvn, wp,
                hid, wbuf, wo, vl, qf, qsend, qrecv, qchip, prob, pnew,
                acc, racc1, racc2, rml2, osum, obf,
                pd, rd, px, rx, pn, rn, pk,
                s_in, s_w, s_k, s_v, s_wo,
                qs, qr, qxs, qxr, qrs, qrr, a1s, a1r, a2s, a2r, m2s, m2r,
                f_s, f_r, n_s, n_r, rxs, rxr):
    sp = lax.axis_index('sp')
    x, c = sp // 2, sp % 2
    sib = 2 * x + (1 - c)
    xp = 2 * (1 - x) + 1 - c
    diag = 2 * (1 - x) + c
    part = (x + c) % 2
    first_pos = sp * SEQ

    def remote(src, dst, ss, rs, peer):
        return pltpu.make_async_remote_copy(src_ref=src, dst_ref=dst, send_sem=ss, recv_sem=rs,
                                            device_id={'sp': peer}, device_id_type=MESH)

    hid_cp = pltpu.make_async_copy(hid_hbm, hid, s_in.at[0])
    wp_cp = pltpu.make_async_copy(wp_hbm, wp, s_in.at[1])
    vl_cp = pltpu.make_async_copy(vl_hbm, vl, s_in.at[2])
    hid_cp.start()

    def head(i, chip):
        return i + chip * (7 - 2 * i)

    def wq_cp(i):
        cols = pl.ds(pl.multiple_of((8 * c + head(i, x)) * HD, HD), HD)
        return pltpu.make_async_copy(wq_hbm.at[:, cols], wbuf.at[i], s_w.at[i % AHEAD])

    def k_cp(g):
        rows = pl.ds(g * CHUNK * SEQ, CHUNK * SEQ)
        return pltpu.make_async_copy(kc_hbm.at[rows], k_ref.at[rows], s_k.at[g])

    def v_cp(g):
        rows = pl.ds(g * CHUNK * SEQ, CHUNK * SEQ)
        return pltpu.make_async_copy(vc_hbm.at[rows], v_ref.at[rows], s_v.at[g])

    def wo_cp(i):
        rows = pl.ds(i * 256, 256)
        return pltpu.make_async_copy(wo_hbm.at[rows], wo.at[rows], s_wo.at[0])

    def start_w(i):
        @pl.when(i < NOWN)
        def _():
            wq_cp(i).start()

        @pl.when((i == NOWN) & (c == 0))
        def _():
            pltpu.make_async_copy(wk_hbm, wbuf.at[NOWN], s_w.at[NOWN % AHEAD]).start()

        @pl.when((i == NOWN) & (c == 1))
        def _():
            pltpu.make_async_copy(wv_hbm, wbuf.at[NOWN], s_w.at[NOWN % AHEAD]).start()

        @pl.when((i > NOWN) & (i < NW + NCH))
        def _():
            k_cp(i - NW).start()
            v_cp(i - NW).start()

    for i in range(AHEAD):
        wq_cp(i).start()
    wp_cp.start()
    vl_cp.start()

    barrier = pltpu.get_barrier_semaphore()
    for peer in (sib, xp):
        pl.semaphore_signal(barrier, inc=1, device_id={'sp': peer}, device_id_type=MESH)

    hid_cp.wait()
    pl.semaphore_wait(barrier, 2)

    def spread(slot, q):
        for h in range(2):
            qf[h, pl.ds(slot, ROWS, stride=HEADS), :] = q[:, h * 128:(h + 1) * 128]

    def slot(i, chip, core):
        h = head(i, chip)
        return 8 * ((core + h // 4) % 2) + 4 * core + h % 4

    def q_core(i, kind):
        return remote(qsend.at[i], qrecv.at[i], qs.at[0], qr.at[kind], sib)

    def q_chip(i):
        return remote(qsend.at[i], qchip.at[i], qxs.at[0], qxr.at[i], xp)

    def q_relay(i):
        return remote(qchip.at[i], qrecv.at[NW + i], qrs.at[0], qrr.at[0], sib)

    def project(i, kind):
        pltpu.make_async_copy(wk_hbm, wbuf.at[i], s_w.at[i % AHEAD]).wait()
        start_w(i + AHEAD)
        res = jnp.dot(hid[...], wbuf[i], preferred_element_type=F32).astype(BF16)
        qsend[i] = res
        q_core(i, kind).start()
        return res.astype(F32)

    def head_step(i, _):
        res = project(i, 0)

        @pl.when(i < SHARED)
        def _():
            q_chip(i).start()

        spread(slot(i, x, c), res)
        return 0

    lax.fori_loop(0, NOWN, head_step, 0)
    def take_shared(i):
        q_chip(i).wait_recv()
        q_relay(i).start()
        spread(slot(i, 1 - x, 1 - c), qchip[i].astype(F32))

    take_shared(0)
    kvn[c] = project(NOWN, 1)
    for i in range(1, SHARED):
        take_shared(i)
    heads = pl.ds(0, NOWN)
    remote(qsend.at[heads], qrecv.at[heads], qs.at[0], qr.at[0], sib).wait_recv()

    def take_head(i, _):
        spread(slot(i, x, 1 - c), qrecv[i].astype(F32))
        return 0

    lax.fori_loop(0, NOWN, take_head, 0)
    remote(qchip, qrecv.at[pl.ds(NW, SHARED)], qrs.at[0], qrr.at[0], sib).wait_recv()
    for i in range(SHARED):
        spread(slot(i, 1 - x, c), qrecv[NW + i].astype(F32))
    q_core(NOWN, 1).wait_recv()
    kvn[1 - c] = qrecv[NOWN].astype(F32)
    wp_cp.wait()
    vl_cp.wait()

    sub = lax.broadcasted_iota(jnp.int32, (8, HD), 0)
    sub1 = lax.broadcasted_iota(jnp.int32, (8, 128), 0)
    lane1 = lax.broadcasted_iota(jnp.int32, (8, 128), 1)
    lane = lax.broadcasted_iota(jnp.int32, (HEADS, SEQ), 1)

    def cache_rows(b):
        return pl.ds(pl.multiple_of(b * SEQ, SEQ), SEQ)

    def weigh(b, j):
        rows = pl.ds(pl.multiple_of(b * HEADS, HEADS), HEADS)
        q = jnp.concatenate([qf[0, rows, :], qf[1, rows, :]], axis=1)
        s = lax.dot_general(q.astype(BF16), k_ref[cache_rows(b), :], (((1,), (1,)), ((), ())),
                            preferred_element_type=F32)
        s_new = jnp.sum(q * kvn[0, pl.ds(b, 1), :], axis=1, keepdims=True)
        here = lane == wp[b] - first_pos
        s = jnp.where(here, s_new, s) * (HD ** -0.5)
        s = jnp.where(lane < vl[b] - first_pos, s, -jnp.inf)
        m = jnp.maximum(jnp.max(s, axis=1, keepdims=True), LOWEST)
        p = jnp.exp(s - m)
        l = jnp.sum(p, axis=1, keepdims=True)
        p_new = jnp.sum(jnp.where(here, p, 0.0), axis=1, keepdims=True)
        mine = slice(j * HEADS, (j + 1) * HEADS)
        prob[mine, :] = jnp.where(here, 0.0, p).astype(BF16)
        pnew[mine, :] = jnp.broadcast_to(p_new, (HEADS, 128))
        return jnp.broadcast_to(m, (HEADS, 128)), jnp.broadcast_to(l, (HEADS, 128))

    def value_sum(b, j):
        mine = slice(j * HEADS, (j + 1) * HEADS)
        o = jnp.dot(prob[mine, :], v_ref[cache_rows(b), :], preferred_element_type=F32)
        p_new = pnew[mine, :]
        return o + jnp.concatenate([p_new, p_new], axis=1) * kvn[1, pl.ds(b, 1), :]

    def pack(t0, t1, low):
        return (jnp.where(low, t0, pltpu.roll(t1, 4, 0)), jnp.where(low, pltpu.roll(t0, 4, 0), t1))

    def chunk_attention(ch, between):
        k_cp(ch).wait()

        @pl.when(ch >= 0)
        def _():
            tiles = [jnp.zeros((8, 128), F32)] * 4
            for p in range(NPAIR):
                m0, l0 = weigh(ch * CHUNK + 2 * p, 2 * p)
                m1, l1 = weigh(ch * CHUNK + 2 * p + 1, 2 * p + 1)
                for core in range(2):
                    r = slice(8 * core, 8 * core + 8)
                    ms = pack(m0[r], m1[r], sub1 < 4)
                    ls = pack(l0[r], l1[r], sub1 < 4)
                    for xd in range(2):
                        t = jnp.where(lane1 == p, ms[xd], tiles[2 * core + xd])
                        tiles[2 * core + xd] = jnp.where(lane1 == p + 64, ls[xd], t)
            for core in range(2):
                acc[core, ch, 2 * CR:, :] = jnp.concatenate(tiles[2 * core:2 * core + 2], axis=1)

        v_cp(ch).wait()

        @pl.when(ch >= 0)
        def _():
            for p in range(NPAIR):
                o0 = value_sum(ch * CHUNK + 2 * p, 2 * p)
                o1 = value_sum(ch * CHUNK + 2 * p + 1, 2 * p + 1)
                for core in range(2):
                    r = slice(8 * core, 8 * core + 8)
                    os = pack(o0[r], o1[r], sub < 4)
                    for xd in range(2):
                        acc[core, ch, xd * CR + p * 8:xd * CR + p * 8 + 8, :] = os[xd]

    def d2d(ch):
        return remote(acc.at[1 - part, ch], racc1.at[ch], a1s.at[0], a1r.at[ch], sib)

    def xlink(ch):
        sums = pl.ds(pl.multiple_of((1 - x) * CR, 8), CR)
        lanes = pl.ds(pl.multiple_of((1 - x) * 128, 128), 128)
        return (remote(acc.at[part, ch, sums], racc2.at[ch], a2s.at[0], a2r.at[ch], xp),
                remote(acc.at[part, ch, pl.ds(2 * CR, 8), lanes], rml2.at[ch], m2s.at[0], m2r.at[ch], xp))

    def scales(mla, mlb):
        top = jnp.maximum(mla, mlb)
        sa, sb = jnp.exp(mla - top), jnp.exp(mlb - top)
        total = mla * pltpu.roll(sa, 64, 1) + mlb * pltpu.roll(sb, 64, 1)
        return top, sa, sb, total

    def merge_core(ch):
        d2d(ch).wait_recv()
        for xd in range(2):
            lanes = slice(xd * 128, xd * 128 + 128)
            top, sa, sb, total = scales(acc[part, ch, 2 * CR:, lanes], racc1[ch, 2 * CR:, lanes])
            acc[part, ch, 2 * CR:, lanes] = jnp.where(lane1 < 64, top, total)
            for p in range(NPAIR):
                r = slice(xd * CR + p * 8, xd * CR + p * 8 + 8)
                acc[part, ch, r, :] = acc[part, ch, r, :] * sa[:, p:p + 1] + racc1[ch, r, :] * sb[:, p:p + 1]
        for desc in xlink(ch):
            desc.start()

    def merge_chip(ch):
        for desc in xlink(ch):
            desc.wait_recv()
        lanes = pl.ds(pl.multiple_of(x * 128, 128), 128)
        top, sa, sb, total = scales(acc[part, ch, 2 * CR:, lanes], rml2[ch])
        inv = pltpu.roll(1.0 / jnp.where(lane1 < 64, 1.0, total), 64, 1)
        sa, sb = sa * inv, sb * inv
        for p in range(NPAIR):
            mine = pl.ds(pl.multiple_of(x * CR + p * 8, 8), 8)
            o = acc[part, ch, mine, :] * sa[:, p:p + 1] + racc2[ch, p * 8:p * 8 + 8, :] * sb[:, p:p + 1]
            for h in range(2):
                osum[h, pl.ds(pl.multiple_of(ch * CR + p * 8, 8), 8), :] = o[:, h * 128:(h + 1) * 128]

    def far_sum(t):
        return remote(pd.at[t], rd.at[t], f_s.at[0], f_r.at[t], sib)

    def near_sum():
        return remote(pn, rn, n_s.at[0], n_r.at[0], sib)

    def chip_sum(t):
        return remote(px.at[t], rx.at[t], rxs.at[0], rxr.at[0], xp)

    def project_block(dst, rows, j):
        cols = pl.ds(pl.multiple_of(j * BLK, BLK), BLK)
        dst[...] = jnp.dot(obf[rows, :], wo[:, cols], preferred_element_type=F32)

    def project_far(t):
        rows = pl.ds(pl.multiple_of(t * OUT, OUT), OUT)
        for r in range(4):
            for h in range(2):
                lanes = slice(r * HD + h * 128, r * HD + (h + 1) * 128)
                obf[rows, lanes] = osum[h, pl.ds(t * 4 * OUT + r, OUT, stride=4), :].astype(BF16)
        project_block(pd.at[t], rows, diag)
        project_block(px.at[t], rows, xp)
        far_sum(t).start()

    def project_near():
        project_block(pn, pl.ds(0, ROWS), sib)
        project_block(pk, pl.ds(0, ROWS), sp)
        near_sum().start()

    def send_far(t):
        far_sum(t).wait_recv()
        px[t] = px[t] + rd[t]
        chip_sum(t).start()

    def pipeline(ch, _):
        def earlier():
            @pl.when(ch >= DIST)
            def _():
                merge_core(ch - DIST)

        @pl.when(ch < 4)
        def _():
            wo_cp(ch).start()

        chunk_attention(ch, earlier)
        d2d(ch).start()
        earlier()
        return 0

    lax.fori_loop(0, NCH, pipeline, 0)

    pltpu.make_async_copy(wo_hbm, wo, s_wo.at[0]).wait()

    def outputs(t, _):
        for u in range(OUT // CHUNK):
            merge_chip(t * (OUT // CHUNK) + u)
        project_far(t)

        @pl.when(t > 0)
        def _():
            send_far(t - 1)
        return 0

    merge_core(NCH - 1)
    lax.fori_loop(0, NOUT, outputs, 0)
    project_near()
    send_far(NOUT - 1)

    remote(qsend, qrecv.at[pl.ds(0, NW)], qs.at[0], qr.at[0], sib).wait_send()
    remote(qchip, qchip, qxs.at[0], qxr.at[0], xp).wait_send()
    remote(qchip, qrecv.at[pl.ds(NW, SHARED)], qrs.at[0], qrr.at[0], sib).wait_send()
    remote(acc.at[1 - part], racc1, a1s.at[0], a1r.at[0], sib).wait_send()
    remote(racc2, racc2, a2s.at[0], a2r.at[0], xp).wait_send()
    remote(rml2, rml2, m2s.at[0], m2r.at[0], xp).wait_send()
    remote(px, rx, f_s.at[0], f_r.at[0], sib).wait_send()
    near_sum().wait_send()

    near_sum().wait_recv()
    remote(px, rx, rxs.at[0], rxr.at[0], xp).wait_recv()
    for t in range(NOUT):
        r = slice(t * OUT, (t + 1) * OUT)
        out_ref[r, :] = ((pk[r, :] + rn[r, :]) + rx[t]).astype(BF16)
    remote(px, rx, rxs.at[0], rxr.at[0], xp).wait_send()


def insert_rows(wp, kvn, first_pos, ref, i, groups):
    row = lax.broadcasted_iota(jnp.int32, (16, HD), 0)
    for b in range(groups.start * GROUP, groups.stop * GROUP):
        pos = wp[b] - first_pos
        base = jnp.clip(pos, 0, SEQ - 1) // 16 * 16
        rows = pl.ds(pl.multiple_of(b * SEQ + base, 16), 16)
        ref[rows, :] = jnp.where(row == pos - base, kvn[i, pl.ds(b, 1), :], ref[rows, :].astype(F32)).astype(BF16)


def copy_group(ref, out, sem, g):
    rows = pl.ds(g * GROUP * SEQ, GROUP * SEQ)
    return pltpu.make_async_copy(ref.at[rows], out.at[rows], sem)


def cache_kernel(wp, kvn, k_in, v_in, k_ref, v_ref, k_out, v_out, sems):
    first_pos = lax.axis_index('sp') * SEQ
    copies = []
    for g in range(9):
        if g < 8:
            insert_rows(wp, kvn, first_pos, k_ref, 0, range(g, g + 1))
        if g >= 1:
            copies.append(copy_group(k_ref, k_out, sems.at[len(copies)], g - 1))
            copies[-1].start()
        if g < 8:
            insert_rows(wp, kvn, first_pos, v_ref, 1, range(g, g + 1))
        if g >= 1:
            if g <= SPLIT:
                copies.append(copy_group(v_ref, v_out, sems.at[len(copies)], g - 1))
                copies[-1].start()
    for cp in copies:
        cp.wait()


def rest_kernel(v_ref, token, v_in, v_out, sems):
    copies = [copy_group(v_ref, v_out, sems.at[g], g) for g in range(SPLIT, 8)]
    for cp in copies:
        cp.start()
    for cp in copies:
        cp.wait()


def join_kernel(b0, b1, b2, b3, out, sems):
    sp = lax.axis_index('sp')
    x, c = sp // 2, sp % 2
    copies = []
    for i, ref in enumerate((b0, b1, b2, b3)):
        j = (sp, 2 * x + 1 - c, 3 - sp, 2 * (1 - x) + c)[i]
        cols = pl.ds(pl.multiple_of(j * BLK, BLK), BLK)
        copies.append(pltpu.make_async_copy(ref, out.at[:, cols], sems.at[i]))
    for cp in copies:
        cp.start()
    for cp in copies:
        cp.wait()


def solution(mesh):
    row_spec = P(('rep', 'dp'), None)
    cache_spec = P(('rep', 'dp'), 'sp', None, None)
    len_spec = P(('rep', 'dp'))

    def local_step(hidden, w_query, w_key, w_value, w_out, k_cache, v_cache, write_pos, valid_len):
        flat = (ROWS * SEQ, HD)
        args = (hidden, w_query, w_key, w_value, w_out, k_cache.reshape(flat), v_cache.reshape(flat),
                write_pos, valid_len)
        args = tuple(pltpu.with_memory_space_constraint(a, pltpu.HBM) for a in args)
        vm = pl.BlockSpec(memory_space=pltpu.VMEM)
        dma = pltpu.SemaphoreType.DMA
        out, k_old, v_old, kv_new, where_to = pl.pallas_call(
            step_kernel,
            out_shape=[pltpu.VMEM((ROWS, BLK), BF16), pltpu.VMEM(flat, BF16), pltpu.VMEM(flat, BF16),
                       pltpu.VMEM((2, ROWS, HD), F32), pltpu.SMEM((ROWS,), jnp.int32)],
            in_specs=[pl.BlockSpec(memory_space=pltpu.HBM)] * 9,
            out_specs=[vm, vm, vm, vm, pl.BlockSpec(memory_space=pltpu.SMEM)],
            scratch_shapes=[
                pltpu.VMEM((ROWS, DIM), BF16),
                pltpu.VMEM((NW, DIM, HD), BF16),
                pltpu.VMEM((BLK, DIM), BF16),
                pltpu.SMEM((ROWS,), jnp.int32),
                pltpu.VMEM((2, ROWS * HEADS, 128), F32),
                pltpu.VMEM((NW, ROWS, HD), BF16),
                pltpu.VMEM((NW + SHARED, ROWS, HD), BF16),
                pltpu.VMEM((SHARED, ROWS, HD), BF16),
                pltpu.VMEM((CHUNK * HEADS, SEQ), BF16),
                pltpu.VMEM((CHUNK * HEADS, 128), F32),
                pltpu.VMEM((2, NCH, 2 * CR + 8, HD), F32),
                pltpu.VMEM((NCH, 2 * CR + 8, HD), F32),
                pltpu.VMEM((NCH, CR, HD), F32),
                pltpu.VMEM((NCH, 8, 128), F32),
                pltpu.VMEM((2, 4 * ROWS, 128), F32),
                pltpu.VMEM((ROWS, BLK), BF16),
                pltpu.VMEM((NOUT, OUT, BLK), F32),
                pltpu.VMEM((NOUT, OUT, BLK), F32),
                pltpu.VMEM((NOUT, OUT, BLK), F32),
                pltpu.VMEM((NOUT, OUT, BLK), F32),
                pltpu.VMEM((ROWS, BLK), F32),
                pltpu.VMEM((ROWS, BLK), F32),
                pltpu.VMEM((ROWS, BLK), F32),
                dma((3,)), dma((AHEAD,)), dma((NCH,)), dma((NCH,)), dma((1,)),
                dma((1,)), dma((2,)), dma((1,)), dma((SHARED,)), dma((1,)), dma((1,)),
                dma((1,)), dma((NCH,)), dma((1,)), dma((NCH,)), dma((1,)), dma((NCH,)),
                dma((1,)), dma((NOUT,)), dma((1,)), dma((1,)), dma((1,)), dma((1,)),
            ],
            compiler_params=pltpu.CompilerParams(
                vmem_limit_bytes=44 * 2 ** 20, collective_id=0, has_side_effects=True),
            name='decode_step',
        )(*args)
        anywhere = pl.BlockSpec(memory_space=pltpu.HBM)
        near = [(i, i ^ 1) for i in range(4)]
        chip = lax.ppermute(out, 'sp', [(i, 3 - i) for i in range(4)])
        core = lax.ppermute(out, 'sp', near)
        far = lax.ppermute(chip, 'sp', near)
        k_full, v_full, k_new, v_new = pl.pallas_call(
            cache_kernel,
            out_shape=[pltpu.VMEM(flat, BF16), pltpu.VMEM(flat, BF16),
                       pltpu.HBM(flat, BF16), pltpu.HBM(flat, BF16)],
            in_specs=[pl.BlockSpec(memory_space=pltpu.SMEM), vm, vm, vm],
            out_specs=[vm, vm, anywhere, anywhere],
            scratch_shapes=[dma((16,))],
            input_output_aliases={2: 0, 3: 1},
            cost_estimate=pl.CostEstimate(flops=2 ** 33, bytes_accessed=2 ** 25, transcendentals=0),
            compiler_params=pltpu.CompilerParams(vmem_limit_bytes=2 ** 20),
            name='cache_update',
        )(where_to, kv_new, k_old, v_old)
        v_new = pl.pallas_call(
            rest_kernel,
            out_shape=pltpu.HBM(flat, BF16),
            in_specs=[vm, pl.BlockSpec(memory_space=pl.ANY), anywhere],
            out_specs=anywhere,
            scratch_shapes=[dma((8,))],
            input_output_aliases={2: 0},
            cost_estimate=pl.CostEstimate(flops=2 ** 33, bytes_accessed=2 ** 24, transcendentals=0),
            compiler_params=pltpu.CompilerParams(vmem_limit_bytes=2 ** 20),
            name='cache_rest',
        )(v_full, chip, v_new)
        others = [pltpu.with_memory_space_constraint(o, pltpu.VMEM) for o in (core, chip, far)]
        attn_out = pl.pallas_call(
            join_kernel,
            out_shape=pltpu.HBM((ROWS, DIM), BF16),
            in_specs=[vm] * 4,
            out_specs=anywhere,
            scratch_shapes=[dma((4,))],
            compiler_params=pltpu.CompilerParams(vmem_limit_bytes=2 ** 20),
            name='join',
        )(out, *others)
        return attn_out, k_new.reshape(k_cache.shape), v_new.reshape(v_cache.shape)

    return jax.shard_map(local_step, mesh=mesh, in_specs=(row_spec, P(), P(), P(), P('sp', None), cache_spec, cache_spec, len_spec, len_spec), out_specs=(row_spec, cache_spec, cache_spec), check_vma=False)
```

```python
import jax
import jax.numpy as jnp
from jax import lax
from jax.experimental import pallas as pl
from jax.experimental.pallas import tpu as pltpu
from jax.sharding import PartitionSpec as P

MESH = pl.DeviceIdType.MESH
F32, BF16 = jnp.float32, jnp.bfloat16
LOWEST = float(jnp.finfo(jnp.float32).min)

ROWS = 64
SEQ = 256
DIM = 4096
HD = 256
HEADS = 16
GROUP = 8
CHUNK = 16
NCH = ROWS // CHUNK
NPAIR = CHUNK // 2
CR = NPAIR * 8
OUT = 16
NOUT = ROWS // OUT
BLK = 1024
SPLIT = 6
AHEAD = 4
SHARED = 3
NOWN = 8 - SHARED
NW = NOWN + 1
DIST = 1


def step_kernel(hid_hbm, wq_hbm, wk_hbm, wv_hbm, wo_hbm, kc_hbm, vc_hbm, wp_hbm, vl_hbm,
                out_ref, k_ref, v_ref, kvn, wp,
                hid, wbuf, wo, vl, qf, qsend, qrecv, qchip, prob, pnew,
                acc, racc1, racc2, rml2, osum, obf,
                pd, rd, px, rx, pn, rn, pk,
                s_in, s_w, s_k, s_v, s_wo,
                qs, qr, qxs, qxr, qrs, qrr, a1s, a1r, a2s, a2r, m2s, m2r,
                f_s, f_r, n_s, n_r, rxs, rxr):
    sp = lax.axis_index('sp')
    x, c = sp // 2, sp % 2
    sib = 2 * x + (1 - c)
    xp = 2 * (1 - x) + 1 - c
    diag = 2 * (1 - x) + c
    part = (x + c) % 2
    first_pos = sp * SEQ

    def remote(src, dst, ss, rs, peer):
        return pltpu.make_async_remote_copy(src_ref=src, dst_ref=dst, send_sem=ss, recv_sem=rs,
                                            device_id={'sp': peer}, device_id_type=MESH)

    hid_cp = pltpu.make_async_copy(hid_hbm, hid, s_in.at[0])
    wp_cp = pltpu.make_async_copy(wp_hbm, wp, s_in.at[1])
    vl_cp = pltpu.make_async_copy(vl_hbm, vl, s_in.at[2])
    hid_cp.start()

    def head(i, chip):
        return i + chip * (7 - 2 * i)

    def wq_cp(i):
        cols = pl.ds(pl.multiple_of((8 * c + head(i, x)) * HD, HD), HD)
        return pltpu.make_async_copy(wq_hbm.at[:, cols], wbuf.at[i], s_w.at[i % AHEAD])

    def k_cp(g):
        rows = pl.ds(g * CHUNK * SEQ, CHUNK * SEQ)
        return pltpu.make_async_copy(kc_hbm.at[rows], k_ref.at[rows], s_k.at[g])

    def v_cp(g):
        rows = pl.ds(g * CHUNK * SEQ, CHUNK * SEQ)
        return pltpu.make_async_copy(vc_hbm.at[rows], v_ref.at[rows], s_v.at[g])

    def wo_cp(i):
        rows = pl.ds(i * 256, 256)
        return pltpu.make_async_copy(wo_hbm.at[rows], wo.at[rows], s_wo.at[0])

    def start_w(i):
        @pl.when(i < NOWN)
        def _():
            wq_cp(i).start()

        @pl.when((i == NOWN) & (c == 0))
        def _():
            pltpu.make_async_copy(wk_hbm, wbuf.at[NOWN], s_w.at[NOWN % AHEAD]).start()

        @pl.when((i == NOWN) & (c == 1))
        def _():
            pltpu.make_async_copy(wv_hbm, wbuf.at[NOWN], s_w.at[NOWN % AHEAD]).start()

        @pl.when((i > NOWN) & (i < NW + NCH))
        def _():
            k_cp(i - NW).start()
            v_cp(i - NW).start()

    for i in range(AHEAD):
        wq_cp(i).start()
    wp_cp.start()
    vl_cp.start()

    barrier = pltpu.get_barrier_semaphore()
    for peer in (sib, xp):
        pl.semaphore_signal(barrier, inc=1, device_id={'sp': peer}, device_id_type=MESH)

    hid_cp.wait()
    pl.semaphore_wait(barrier, 2)

    def spread(slot, q):
        for h in range(2):
            qf[h, pl.ds(slot, ROWS, stride=HEADS), :] = q[:, h * 128:(h + 1) * 128]

    def slot(i, chip, core):
        h = head(i, chip)
        return 8 * ((core + h // 4) % 2) + 4 * core + h % 4

    def q_core(i, kind):
        return remote(qsend.at[i], qrecv.at[i], qs.at[0], qr.at[kind], sib)

    def q_chip(i):
        return remote(qsend.at[i], qchip.at[i], qxs.at[0], qxr.at[i], xp)

    def q_relay(i):
        return remote(qchip.at[i], qrecv.at[NW + i], qrs.at[0], qrr.at[0], sib)

    def project(i, kind):
        pltpu.make_async_copy(wk_hbm, wbuf.at[i], s_w.at[i % AHEAD]).wait()
        start_w(i + AHEAD)
        res = jnp.dot(hid[...], wbuf[i], preferred_element_type=F32).astype(BF16)
        qsend[i] = res
        q_core(i, kind).start()
        return res.astype(F32)

    def head_step(i, _):
        res = project(i, 0)

        @pl.when(i < SHARED)
        def _():
            q_chip(i).start()

        spread(slot(i, x, c), res)
        return 0

    lax.fori_loop(0, NOWN, head_step, 0)
    def take_shared(i):
        q_chip(i).wait_recv()
        q_relay(i).start()
        spread(slot(i, 1 - x, 1 - c), qchip[i].astype(F32))

    take_shared(0)
    kvn[c] = project(NOWN, 1)
    for i in range(1, SHARED):
        take_shared(i)
    heads = pl.ds(0, NOWN)
    remote(qsend.at[heads], qrecv.at[heads], qs.at[0], qr.at[0], sib).wait_recv()

    def take_head(i, _):
        spread(slot(i, x, 1 - c), qrecv[i].astype(F32))
        return 0

    lax.fori_loop(0, NOWN, take_head, 0)
    remote(qchip, qrecv.at[pl.ds(NW, SHARED)], qrs.at[0], qrr.at[0], sib).wait_recv()
    for i in range(SHARED):
        spread(slot(i, 1 - x, c), qrecv[NW + i].astype(F32))
    q_core(NOWN, 1).wait_recv()
    kvn[1 - c] = qrecv[NOWN].astype(F32)
    wp_cp.wait()
    vl_cp.wait()

    sub = lax.broadcasted_iota(jnp.int32, (8, HD), 0)
    sub1 = lax.broadcasted_iota(jnp.int32, (8, 128), 0)
    lane1 = lax.broadcasted_iota(jnp.int32, (8, 128), 1)
    lane = lax.broadcasted_iota(jnp.int32, (HEADS, SEQ), 1)

    def cache_rows(b):
        return pl.ds(pl.multiple_of(b * SEQ, SEQ), SEQ)

    def weigh(b, j):
        rows = pl.ds(pl.multiple_of(b * HEADS, HEADS), HEADS)
        q = jnp.concatenate([qf[0, rows, :], qf[1, rows, :]], axis=1)
        s = lax.dot_general(q.astype(BF16), k_ref[cache_rows(b), :], (((1,), (1,)), ((), ())),
                            preferred_element_type=F32)
        s_new = jnp.sum(q * kvn[0, pl.ds(b, 1), :], axis=1, keepdims=True)
        here = lane == wp[b] - first_pos
        s = jnp.where(here, s_new, s) * (HD ** -0.5)
        s = jnp.where(lane < vl[b] - first_pos, s, -jnp.inf)
        m = jnp.maximum(jnp.max(s, axis=1, keepdims=True), LOWEST)
        p = jnp.exp(s - m)
        l = jnp.sum(p, axis=1, keepdims=True)
        p_new = jnp.sum(jnp.where(here, p, 0.0), axis=1, keepdims=True)
        mine = slice(j * HEADS, (j + 1) * HEADS)
        prob[mine, :] = jnp.where(here, 0.0, p).astype(BF16)
        pnew[mine, :] = jnp.broadcast_to(p_new, (HEADS, 128))
        return jnp.broadcast_to(m, (HEADS, 128)), jnp.broadcast_to(l, (HEADS, 128))

    def value_sum(b, j):
        mine = slice(j * HEADS, (j + 1) * HEADS)
        o = jnp.dot(prob[mine, :], v_ref[cache_rows(b), :], preferred_element_type=F32)
        p_new = pnew[mine, :]
        return o + jnp.concatenate([p_new, p_new], axis=1) * kvn[1, pl.ds(b, 1), :]

    def pack(t0, t1, low):
        return (jnp.where(low, t0, pltpu.roll(t1, 4, 0)), jnp.where(low, pltpu.roll(t0, 4, 0), t1))

    def chunk_attention(ch, between):
        k_cp(ch).wait()

        @pl.when(ch >= 0)
        def _():
            tiles = [jnp.zeros((8, 128), F32)] * 4
            for p in range(NPAIR):
                m0, l0 = weigh(ch * CHUNK + 2 * p, 2 * p)
                m1, l1 = weigh(ch * CHUNK + 2 * p + 1, 2 * p + 1)
                for core in range(2):
                    r = slice(8 * core, 8 * core + 8)
                    ms = pack(m0[r], m1[r], sub1 < 4)
                    ls = pack(l0[r], l1[r], sub1 < 4)
                    for xd in range(2):
                        t = jnp.where(lane1 == p, ms[xd], tiles[2 * core + xd])
                        tiles[2 * core + xd] = jnp.where(lane1 == p + 64, ls[xd], t)
            for core in range(2):
                acc[core, ch, 2 * CR:, :] = jnp.concatenate(tiles[2 * core:2 * core + 2], axis=1)

        v_cp(ch).wait()

        @pl.when(ch >= 0)
        def _():
            for p in range(NPAIR):
                o0 = value_sum(ch * CHUNK + 2 * p, 2 * p)
                o1 = value_sum(ch * CHUNK + 2 * p + 1, 2 * p + 1)
                for core in range(2):
                    r = slice(8 * core, 8 * core + 8)
                    os = pack(o0[r], o1[r], sub < 4)
                    for xd in range(2):
                        acc[core, ch, xd * CR + p * 8:xd * CR + p * 8 + 8, :] = os[xd]

    def d2d(ch):
        return remote(acc.at[1 - part, ch], racc1.at[ch], a1s.at[0], a1r.at[ch], sib)

    def xlink(ch):
        sums = pl.ds(pl.multiple_of((1 - x) * CR, 8), CR)
        lanes = pl.ds(pl.multiple_of((1 - x) * 128, 128), 128)
        return (remote(acc.at[part, ch, sums], racc2.at[ch], a2s.at[0], a2r.at[ch], xp),
                remote(acc.at[part, ch, pl.ds(2 * CR, 8), lanes], rml2.at[ch], m2s.at[0], m2r.at[ch], xp))

    def scales(mla, mlb):
        top = jnp.maximum(mla, mlb)
        sa, sb = jnp.exp(mla - top), jnp.exp(mlb - top)
        total = mla * pltpu.roll(sa, 64, 1) + mlb * pltpu.roll(sb, 64, 1)
        return top, sa, sb, total

    def merge_core(ch):
        d2d(ch).wait_recv()
        for xd in range(2):
            lanes = slice(xd * 128, xd * 128 + 128)
            top, sa, sb, total = scales(acc[part, ch, 2 * CR:, lanes], racc1[ch, 2 * CR:, lanes])
            acc[part, ch, 2 * CR:, lanes] = jnp.where(lane1 < 64, top, total)
            for p in range(NPAIR):
                r = slice(xd * CR + p * 8, xd * CR + p * 8 + 8)
                acc[part, ch, r, :] = acc[part, ch, r, :] * sa[:, p:p + 1] + racc1[ch, r, :] * sb[:, p:p + 1]
        for desc in xlink(ch):
            desc.start()

    def merge_chip(ch):
        for desc in xlink(ch):
            desc.wait_recv()
        lanes = pl.ds(pl.multiple_of(x * 128, 128), 128)
        top, sa, sb, total = scales(acc[part, ch, 2 * CR:, lanes], rml2[ch])
        inv = pltpu.roll(1.0 / jnp.where(lane1 < 64, 1.0, total), 64, 1)
        sa, sb = sa * inv, sb * inv
        for p in range(NPAIR):
            mine = pl.ds(pl.multiple_of(x * CR + p * 8, 8), 8)
            o = acc[part, ch, mine, :] * sa[:, p:p + 1] + racc2[ch, p * 8:p * 8 + 8, :] * sb[:, p:p + 1]
            for h in range(2):
                osum[h, pl.ds(pl.multiple_of(ch * CR + p * 8, 8), 8), :] = o[:, h * 128:(h + 1) * 128]

    def far_sum(t):
        return remote(pd.at[t], rd.at[t], f_s.at[0], f_r.at[t], sib)

    def near_sum():
        return remote(pn, rn, n_s.at[0], n_r.at[0], sib)

    def chip_sum(t):
        return remote(px.at[t], rx.at[t], rxs.at[0], rxr.at[0], xp)

    def project_block(dst, rows, j):
        cols = pl.ds(pl.multiple_of(j * BLK, BLK), BLK)
        dst[...] = jnp.dot(obf[rows, :], wo[:, cols], preferred_element_type=F32)

    def project_far(t):
        rows = pl.ds(pl.multiple_of(t * OUT, OUT), OUT)
        for r in range(4):
            for h in range(2):
                lanes = slice(r * HD + h * 128, r * HD + (h + 1) * 128)
                obf[rows, lanes] = osum[h, pl.ds(t * 4 * OUT + r, OUT, stride=4), :].astype(BF16)
        project_block(pd.at[t], rows, diag)
        project_block(px.at[t], rows, xp)
        far_sum(t).start()

    def project_near():
        project_block(pn, pl.ds(0, ROWS), sib)
        project_block(pk, pl.ds(0, ROWS), sp)
        near_sum().start()

    def send_far(t):
        far_sum(t).wait_recv()
        px[t] = px[t] + rd[t]
        chip_sum(t).start()

    def pipeline(ch, _):
        def earlier():
            @pl.when(ch >= DIST)
            def _():
                merge_core(ch - DIST)

        @pl.when(ch < 4)
        def _():
            wo_cp(ch).start()

        chunk_attention(ch, earlier)
        d2d(ch).start()
        earlier()
        return 0

    lax.fori_loop(0, NCH, pipeline, 0)

    pltpu.make_async_copy(wo_hbm, wo, s_wo.at[0]).wait()

    def outputs(t, _):
        for u in range(OUT // CHUNK):
            merge_chip(t * (OUT // CHUNK) + u)
        project_far(t)

        @pl.when(t > 0)
        def _():
            send_far(t - 1)
        return 0

    merge_core(NCH - 1)
    lax.fori_loop(0, NOUT, outputs, 0)
    project_near()
    send_far(NOUT - 1)

    remote(qsend, qrecv.at[pl.ds(0, NW)], qs.at[0], qr.at[0], sib).wait_send()
    remote(qchip, qchip, qxs.at[0], qxr.at[0], xp).wait_send()
    remote(qchip, qrecv.at[pl.ds(NW, SHARED)], qrs.at[0], qrr.at[0], sib).wait_send()
    remote(acc.at[1 - part], racc1, a1s.at[0], a1r.at[0], sib).wait_send()
    remote(racc2, racc2, a2s.at[0], a2r.at[0], xp).wait_send()
    remote(rml2, rml2, m2s.at[0], m2r.at[0], xp).wait_send()
    remote(px, rx, f_s.at[0], f_r.at[0], sib).wait_send()
    near_sum().wait_send()

    near_sum().wait_recv()
    remote(px, rx, rxs.at[0], rxr.at[0], xp).wait_recv()
    for t in range(NOUT):
        r = slice(t * OUT, (t + 1) * OUT)
        out_ref[r, :] = ((pk[r, :] + rn[r, :]) + rx[t]).astype(BF16)
    remote(px, rx, rxs.at[0], rxr.at[0], xp).wait_send()


def insert_rows(wp, kvn, first_pos, ref, i, groups):
    row = lax.broadcasted_iota(jnp.int32, (16, HD), 0)
    for b in range(groups.start * GROUP, groups.stop * GROUP):
        pos = wp[b] - first_pos
        base = jnp.clip(pos, 0, SEQ - 1) // 16 * 16
        rows = pl.ds(pl.multiple_of(b * SEQ + base, 16), 16)
        ref[rows, :] = jnp.where(row == pos - base, kvn[i, pl.ds(b, 1), :], ref[rows, :].astype(F32)).astype(BF16)


def copy_group(ref, out, sem, g):
    rows = pl.ds(g * GROUP * SEQ, GROUP * SEQ)
    return pltpu.make_async_copy(ref.at[rows], out.at[rows], sem)


def cache_kernel(wp, kvn, k_in, v_in, k_ref, v_ref, k_out, v_out, sems):
    first_pos = lax.axis_index('sp') * SEQ
    copies = []
    insert_rows(wp, kvn, first_pos, k_ref, 0, range(0, 1))
    for g in range(8):
        if g < 7:
            insert_rows(wp, kvn, first_pos, k_ref, 0, range(g + 1, g + 2))
        copies.append(copy_group(k_ref, k_out, sems.at[len(copies)], g))
        copies[-1].start()
        insert_rows(wp, kvn, first_pos, v_ref, 1, range(g, g + 1))
        if 1 <= g <= SPLIT:
            copies.append(copy_group(v_ref, v_out, sems.at[len(copies)], g - 1))
            copies[-1].start()
    for cp in copies:
        cp.wait()


def rest_kernel(v_ref, token, v_in, v_out, sems):
    copies = [copy_group(v_ref, v_out, sems.at[g], g) for g in range(SPLIT, 8)]
    for cp in copies:
        cp.start()
    for cp in copies:
        cp.wait()


def join_kernel(b0, b1, b2, b3, out, sems):
    sp = lax.axis_index('sp')
    x, c = sp // 2, sp % 2
    copies = []
    for i, ref in enumerate((b0, b1, b2, b3)):
        j = (sp, 2 * x + 1 - c, 3 - sp, 2 * (1 - x) + c)[i]
        cols = pl.ds(pl.multiple_of(j * BLK, BLK), BLK)
        copies.append(pltpu.make_async_copy(ref, out.at[:, cols], sems.at[i]))
    for cp in copies:
        cp.start()
    for cp in copies:
        cp.wait()


def solution(mesh):
    row_spec = P(('rep', 'dp'), None)
    cache_spec = P(('rep', 'dp'), 'sp', None, None)
    len_spec = P(('rep', 'dp'))

    def local_step(hidden, w_query, w_key, w_value, w_out, k_cache, v_cache, write_pos, valid_len):
        flat = (ROWS * SEQ, HD)
        args = (hidden, w_query, w_key, w_value, w_out, k_cache.reshape(flat), v_cache.reshape(flat),
                write_pos, valid_len)
        args = tuple(pltpu.with_memory_space_constraint(a, pltpu.HBM) for a in args)
        vm = pl.BlockSpec(memory_space=pltpu.VMEM)
        dma = pltpu.SemaphoreType.DMA
        out, k_old, v_old, kv_new, where_to = pl.pallas_call(
            step_kernel,
            out_shape=[pltpu.VMEM((ROWS, BLK), BF16), pltpu.VMEM(flat, BF16), pltpu.VMEM(flat, BF16),
                       pltpu.VMEM((2, ROWS, HD), F32), pltpu.SMEM((ROWS,), jnp.int32)],
            in_specs=[pl.BlockSpec(memory_space=pltpu.HBM)] * 9,
            out_specs=[vm, vm, vm, vm, pl.BlockSpec(memory_space=pltpu.SMEM)],
            scratch_shapes=[
                pltpu.VMEM((ROWS, DIM), BF16),
                pltpu.VMEM((NW, DIM, HD), BF16),
                pltpu.VMEM((BLK, DIM), BF16),
                pltpu.SMEM((ROWS,), jnp.int32),
                pltpu.VMEM((2, ROWS * HEADS, 128), F32),
                pltpu.VMEM((NW, ROWS, HD), BF16),
                pltpu.VMEM((NW + SHARED, ROWS, HD), BF16),
                pltpu.VMEM((SHARED, ROWS, HD), BF16),
                pltpu.VMEM((CHUNK * HEADS, SEQ), BF16),
                pltpu.VMEM((CHUNK * HEADS, 128), F32),
                pltpu.VMEM((2, NCH, 2 * CR + 8, HD), F32),
                pltpu.VMEM((NCH, 2 * CR + 8, HD), F32),
                pltpu.VMEM((NCH, CR, HD), F32),
                pltpu.VMEM((NCH, 8, 128), F32),
                pltpu.VMEM((2, 4 * ROWS, 128), F32),
                pltpu.VMEM((ROWS, BLK), BF16),
                pltpu.VMEM((NOUT, OUT, BLK), F32),
                pltpu.VMEM((NOUT, OUT, BLK), F32),
                pltpu.VMEM((NOUT, OUT, BLK), F32),
                pltpu.VMEM((NOUT, OUT, BLK), F32),
                pltpu.VMEM((ROWS, BLK), F32),
                pltpu.VMEM((ROWS, BLK), F32),
                pltpu.VMEM((ROWS, BLK), F32),
                dma((3,)), dma((AHEAD,)), dma((NCH,)), dma((NCH,)), dma((1,)),
                dma((1,)), dma((2,)), dma((1,)), dma((SHARED,)), dma((1,)), dma((1,)),
                dma((1,)), dma((NCH,)), dma((1,)), dma((NCH,)), dma((1,)), dma((NCH,)),
                dma((1,)), dma((NOUT,)), dma((1,)), dma((1,)), dma((1,)), dma((1,)),
            ],
            compiler_params=pltpu.CompilerParams(
                vmem_limit_bytes=44 * 2 ** 20, collective_id=0, has_side_effects=True),
            name='decode_step',
        )(*args)
        anywhere = pl.BlockSpec(memory_space=pltpu.HBM)
        near = [(i, i ^ 1) for i in range(4)]
        chip = lax.ppermute(out, 'sp', [(i, 3 - i) for i in range(4)])
        core = lax.ppermute(out, 'sp', near)
        far = lax.ppermute(chip, 'sp', near)
        k_full, v_full, k_new, v_new = pl.pallas_call(
            cache_kernel,
            out_shape=[pltpu.VMEM(flat, BF16), pltpu.VMEM(flat, BF16),
                       pltpu.HBM(flat, BF16), pltpu.HBM(flat, BF16)],
            in_specs=[pl.BlockSpec(memory_space=pltpu.SMEM), vm, vm, vm],
            out_specs=[vm, vm, anywhere, anywhere],
            scratch_shapes=[dma((16,))],
            input_output_aliases={2: 0, 3: 1},
            cost_estimate=pl.CostEstimate(flops=2 ** 33, bytes_accessed=2 ** 25, transcendentals=0),
            compiler_params=pltpu.CompilerParams(vmem_limit_bytes=2 ** 20),
            name='cache_update',
        )(where_to, kv_new, k_old, v_old)
        v_new = pl.pallas_call(
            rest_kernel,
            out_shape=pltpu.HBM(flat, BF16),
            in_specs=[vm, pl.BlockSpec(memory_space=pl.ANY), anywhere],
            out_specs=anywhere,
            scratch_shapes=[dma((8,))],
            input_output_aliases={2: 0},
            cost_estimate=pl.CostEstimate(flops=2 ** 33, bytes_accessed=2 ** 24, transcendentals=0),
            compiler_params=pltpu.CompilerParams(vmem_limit_bytes=2 ** 20),
            name='cache_rest',
        )(v_full, chip, v_new)
        others = [pltpu.with_memory_space_constraint(o, pltpu.VMEM) for o in (core, chip, far)]
        attn_out = pl.pallas_call(
            join_kernel,
            out_shape=pltpu.HBM((ROWS, DIM), BF16),
            in_specs=[vm] * 4,
            out_specs=anywhere,
            scratch_shapes=[dma((4,))],
            compiler_params=pltpu.CompilerParams(vmem_limit_bytes=2 ** 20),
            name='join',
        )(out, *others)
        return attn_out, k_new.reshape(k_cache.shape), v_new.reshape(v_cache.shape)

    return jax.shard_map(local_step, mesh=mesh, in_specs=(row_spec, P(), P(), P(), P('sp', None), cache_spec, cache_spec, len_spec, len_spec), out_specs=(row_spec, cache_spec, cache_spec), check_vma=False)
```
